256 devices in a mesh: outer: 8 (over x, y_hi), inner: 32 (over y_lo, z, core).
Axes of the slice: x: 4, y: 4 (y_hi: 2, y_lo: 2; y = y_hi * 2 + y_lo), z: 8, core: 2. Of those that a mesh axis runs over, the one named last changes fastest.
Arguments:
- tokens: bfloat16 [32768, 4096], P('inner', 'outer'), may hold values from -6 to 6
- cotangent: bfloat16 [32768, 4096], P('inner', 'outer'), may hold values from -0.03125 to 0.03125
- weight_cache: bfloat16 [4096, 4096], P(None, 'outer'), may hold values from -0.09375 to 0.09375
- weight_delta: bfloat16 [4096, 4096], P('inner', 'outer'), may hold values from -0.078125 to 0.078125
- sign_bits: int32 [4096], P('outer'), may hold values from 0 to 1
- master: float32 [4096, 4096], P('inner', 'outer'), may hold values from -1.5 to 1.5
- moment: float32 [4096, 4096], P('inner', 'outer'), may hold values from -6 to 6
- variance: float32 [4096, 4096], P('inner', 'outer'), may hold values from 0.25 to 4
Outputs:
- activation: float32 [32768, 4096], P('inner', 'outer')
- new_master: float32 [4096, 4096], P('inner', 'outer')
- new_moment: float32 [4096, 4096], P('inner', 'outer')
- new_variance: float32 [4096, 4096], P('inner', 'outer')
- block_scales: float32 [4096, 32], P('inner', 'outer')
The draws below stay inside these ranges and needn't reach their ends.
All inputs are finite; a program needn't handle non-finite values.
Results may differ from the reference program's by a relative error of at most 0.003.
Values may be sent and summed in bfloat16 or wider, within the bound.
A program may use at most 128 MiB of HBM per device.

```python
import math
import jax
import jax.numpy as jnp
from jax import lax

IN_FEAT = 4096
OUT_FEAT = 4096
BLOCK = 128
TOKENS = 32768


def place_ends(result, key, least, largest):
    longest = result.shape.index(max(result.shape))
    spots = []
    for shift in (0, 1):
        where = [jax.random.randint(jax.random.fold_in(key, axis), (), 0, length) for axis, length in enumerate(result.shape)]
        where[longest] = (where[longest] + shift) % result.shape[longest]
        spots.append(tuple(where))
    return result.at[spots[0]].set(least).at[spots[1]].set(largest)


def spiked(drawn, stream_key, source, target, blocks, factor):
    def block_of(position):
        return (jnp.arange(drawn.shape[position]) // (drawn.shape[position] // blocks)).reshape((-1,) + (1,) * (drawn.ndim - 1 - position))

    near = jax.random.permutation(stream_key, blocks)[block_of(target)]
    other_side = (block_of(target) + blocks // 2) % blocks
    return jnp.where((block_of(source) == near) | (block_of(source) == other_side), factor * drawn, drawn)


def shard_levels(stream_key, dims, pieces, smallest, high):
    level, own = 1.0, jax.random.fold_in(stream_key, 6)
    for dim, parts in pieces:
        heights = jnp.exp(jax.random.uniform(jax.random.fold_in(own, dim), (parts,), jnp.float32, smallest / len(pieces), high / len(pieces)))
        level = level * jnp.repeat(heights, dims[dim] // parts).reshape([-1 if axis == dim else 1 for axis in range(len(dims))])
    return level


def scatter_about(key, extent, scale, reach, shards=(), kind=jnp.bfloat16):
    array = jax.random.normal(key, extent, jnp.float32) * scale
    if len(shards) > 0:
        array = shard_levels(key, extent, shards, -0.22, 0.18) * array
    return jnp.clip(array, min=-reach, max=reach).astype(kind)


def heavy_noise(key, shape, width, reach, split, heavy, held_as=jnp.bfloat16):
    result = width * jax.random.normal(key, shape, jnp.float32)
    if split:
        result = result * shard_levels(key, shape, split, -0.22, 0.18)
    return jnp.clip(spiked(result, jax.random.fold_in(key, 3), *heavy), -reach, reach).astype(held_as)


def setup_inputs(seed: int = 0) -> dict:
    arg_keys = jax.random.split(jax.random.key(seed), 9)
    return {
        "tokens": heavy_noise(arg_keys[0], (TOKENS, IN_FEAT), 1.0, 6.0, ((0, 32), (1, 8)), (0, 1, 32, 2.75)),
        "cotangent": scatter_about(arg_keys[1], (TOKENS, OUT_FEAT), TOKENS ** -0.5, 0.03125, ((0, 32), (1, 8))),
        "weight_cache": scatter_about(arg_keys[2], (IN_FEAT, OUT_FEAT), IN_FEAT ** -0.5, 0.09375, ((1, 8),)),
        "weight_delta": scatter_about(arg_keys[3], (IN_FEAT, OUT_FEAT), 0.005, 0.078125, ((0, 32), (1, 8))),
        "sign_bits": place_ends(jax.random.randint(arg_keys[4], (OUT_FEAT,), 0, 2), jax.random.fold_in(arg_keys[4], 1), 0, 1).astype(jnp.int32),
        "master": scatter_about(arg_keys[5], (IN_FEAT, OUT_FEAT), 0.1, 1.5, ((0, 32), (1, 8)), jnp.float32),
        "moment": scatter_about(arg_keys[6], (IN_FEAT, OUT_FEAT), 0.5, 6.0, ((0, 32), (1, 8)), jnp.float32),
        "variance": jnp.clip(jnp.exp(math.log(4.0) - 2.7725887 * jax.random.uniform(arg_keys[7], (IN_FEAT, OUT_FEAT), jnp.float32) ** shard_levels(arg_keys[7], (IN_FEAT, OUT_FEAT), ((0, 32), (1, 8)), -0.2, 0.2)), 0.25, 4.0),
    }


def hadamard_table(length):
    first = jnp.arange(length, dtype=jnp.int32)[:, None]
    second = jnp.arange(length, dtype=jnp.int32)[None, :]
    common = jnp.bitwise_and(first, second)
    parity = jnp.zeros((length, length), jnp.int32)
    for place in range(length.bit_length() - 1):
        parity = parity + jnp.bitwise_and(jnp.right_shift(common, place), 1)
    return (1 - 2 * (parity % 2)).astype(jnp.float32) / jnp.sqrt(jnp.float32(length))

def smooth(values, signs, table):
    height = values.shape[0]
    blocks = values.reshape(height, -1, table.shape[0]) * signs.reshape(-1, table.shape[0])
    mixed = jnp.einsum('rbk,kj->rbj', blocks, table, precision=lax.Precision.HIGHEST)
    return mixed.reshape(height, -1)

def unsmooth(values, signs, table):
    height = values.shape[0]
    blocks = values.reshape(height, -1, table.shape[0])
    mixed = jnp.einsum('rbj,jk->rbk', blocks, table, precision=lax.Precision.HIGHEST)
    return (mixed * signs.reshape(-1, table.shape[0])).reshape(height, -1)

def reference(tokens, cotangent, weight_cache, weight_delta, sign_bits, master, moment, variance):
    weight = (weight_cache.astype(jnp.float32) + weight_delta.astype(jnp.float32)).astype(jnp.bfloat16)
    activation = jnp.dot(tokens, weight, preferred_element_type=jnp.float32)
    gradient = lax.dot_general(tokens, cotangent, (((0,), (0,)), ((), ())), preferred_element_type=jnp.float32)
    table = hadamard_table(BLOCK)
    signs = (1 - 2 * sign_bits).astype(jnp.float32)
    smoothed = smooth(gradient, signs, table)
    block_scales = lax.optimization_barrier(jnp.max(jnp.abs(smoothed.reshape(IN_FEAT, -1, BLOCK)), axis=2))
    restored = unsmooth(smoothed, signs, table)
    new_moment = 0.9 * moment + 0.1 * restored
    new_variance = 0.95 * variance + 0.05 * restored * restored
    corrected = new_moment / (1.0 - 0.9 ** 10)
    spread = jnp.sqrt(new_variance / (1.0 - 0.95 ** 10)) + 1e-08
    new_master = master - 0.01 * (corrected / spread + 0.1 * master)
    return (activation, new_master, new_moment, new_variance, block_scales)
```

```python
import functools

import jax
import jax.numpy as jnp
import numpy as np
from jax import lax
from jax.experimental import pallas as pl
from jax.experimental.pallas import tpu as pltpu
from jax.sharding import Mesh
from jax.sharding import PartitionSpec as P

BLOCK = 128
OUTER = ("x", "yh")
INNER = ("yl", "z", "c")
NX, NZ = 4, 8
HALF = 256
MESH = pl.DeviceIdType.MESH
F32, BF16 = jnp.float32, jnp.bfloat16


def transport(
    tokens, cotangent, cache, delta,
    act, grad,
    tok, cot, cot_t, weight, dbuf, gbuf, grcv, zsnd, zrcv, zloc, ysnd, yrcv,
    load_sem, tok_send, tok_recv, d2d_send, d2d_recv, z_send, z_recv, y_send, y_recv,
    dy_sem, dz_send, dz_recv, dc_send, dc_recv,
):
    x, yh, yl = lax.axis_index("x"), lax.axis_index("yh"), lax.axis_index("yl")
    z, c = lax.axis_index("z"), lax.axis_index("c")
    right, left = {"x": (x + 1) % NX}, {"x": (x + 3) % NX}
    across, beside, sibling = {"yh": 1 - yh}, {"yl": 1 - yl}, {"c": 1 - c}
    up, down = {"z": (z + 1) % NZ}, {"z": (z + 7) % NZ}

    def slot(dx, dy, half):
        row = yh if dy == 0 else 1 - yh
        return 4 * ((x + dx) % NX) + 2 * row + half

    own_a, own_b = slot(0, 0, 0), slot(0, 0, 1)
    l_a, l_b, r_a, r_b = slot(3, 0, 0), slot(3, 0, 1), slot(1, 0, 0), slot(1, 0, 1)
    ll_a, ll_b = slot(2, 0, 0), slot(2, 0, 1)
    p_a, p_b = slot(0, 1, 0), slot(0, 1, 1)
    pl_a, pl_b, pr_a, pr_b = slot(3, 1, 0), slot(3, 1, 1), slot(1, 1, 0), slot(1, 1, 1)
    pll_a, pll_b = slot(2, 1, 0), slot(2, 1, 1)

    load_a = pltpu.make_async_copy(tokens.at[:, pl.ds(0, HALF)], tok.at[own_a], load_sem.at[0])
    load_b = pltpu.make_async_copy(tokens.at[:, pl.ds(HALF, HALF)], tok.at[own_b], load_sem.at[1])
    load_cot = pltpu.make_async_copy(cotangent, cot, load_sem.at[2])
    load_delta = pltpu.make_async_copy(delta, dbuf.at[z, c, yl], load_sem.at[3])
    load_cache = pltpu.make_async_copy(cache, weight, load_sem.at[4])
    for copy in (load_a, load_b, load_cot, load_delta, load_cache):
        copy.start()

    barrier = pltpu.get_barrier_semaphore()
    peers = [right, left, across, beside, sibling]
    peers += [{"z": (z + step) % NZ} for step in range(1, NZ)]
    for peer in peers:
        pl.semaphore_signal(barrier, inc=1, device_id=peer, device_id_type=MESH)
    pl.semaphore_wait(barrier, len(peers))

    way = {"right": (0, right), "left": (1, left), "across": (2, across)}

    def token_copy(place, direction):
        lane, peer = way[direction]
        return pltpu.make_async_remote_copy(
            src_ref=tok.at[place], dst_ref=tok.at[place],
            send_sem=tok_send.at[lane, place], recv_sem=tok_recv.at[place],
            device_id=peer, device_id_type=MESH,
        )

    sent = []

    def send(place, direction):
        token_copy(place, direction).start()
        sent.append((place, direction))

    def arrived(place):
        token_copy(place, "right").wait_recv()

    def d2d_copy(place):
        return pltpu.make_async_remote_copy(
            src_ref=gbuf.at[place, 1 - c], dst_ref=grcv.at[place],
            send_sem=d2d_send.at[place], recv_sem=d2d_recv.at[place],
            device_id=sibling, device_id_type=MESH,
        )

    def target(place):
        block = place // 2
        return block // 4, 2 * (block % 4) + place % 2

    def z_copy(place):
        rows, depth = target(place)
        return pltpu.make_async_remote_copy(
            src_ref=zsnd.at[place], dst_ref=zrcv.at[rows, z],
            send_sem=z_send.at[place], recv_sem=z_recv.at[rows, z],
            device_id={"z": depth}, device_id_type=MESH,
        )

    def pick(places, i):
        value = places[0]
        for k in range(1, len(places)):
            value = jnp.where(i == k, places[k], value)
        return value

    def gradients(*places):
        def product(i, carry):
            place = pick(places, i)
            terms = jnp.dot(cot_t[...], tok[place], preferred_element_type=F32)
            gbuf[place, 0] = terms[:, :BLOCK]
            gbuf[place, 1] = terms[:, BLOCK:]
            d2d_copy(place).start()
            return carry

        def merge(i, carry):
            place = pick(places, i)
            d2d_copy(place).wait_recv()
            total = gbuf[place, c] + grcv[place]
            zsnd[place] = total.astype(BF16)
            rows, depth = target(place)

            @pl.when(depth != z)
            def _():
                z_copy(place).start()

            @pl.when(depth == z)
            def _():
                zloc[rows] = total

            return carry

        lax.fori_loop(0, len(places), product, 0)
        lax.fori_loop(0, len(places), merge, 0)

    def dz_copy(origin, lane, peer):
        return pltpu.make_async_remote_copy(
            src_ref=dbuf.at[origin, c], dst_ref=dbuf.at[origin, c],
            send_sem=dz_send.at[lane, origin], recv_sem=dz_recv.at[origin],
            device_id=peer, device_id_type=MESH,
        )

    def dc_copy(origin):
        return pltpu.make_async_remote_copy(
            src_ref=dbuf.at[origin, c], dst_ref=dbuf.at[origin, c],
            send_sem=dc_send.at[origin], recv_sem=dc_recv.at[origin],
            device_id=sibling, device_id_type=MESH,
        )

    dy_copy = pltpu.make_async_remote_copy(
        src_ref=dbuf.at[z, c, yl], dst_ref=dbuf.at[z, c, yl],
        send_sem=dy_sem.at[0], recv_sem=dy_sem.at[1],
        device_id=beside, device_id_type=MESH,
    )
    dy_in = pltpu.make_async_remote_copy(
        src_ref=dbuf.at[z, c, 1 - yl], dst_ref=dbuf.at[z, c, 1 - yl],
        send_sem=dy_sem.at[0], recv_sem=dy_sem.at[1],
        device_id=beside, device_id_type=MESH,
    )
    dz_sent = []

    def delta_step(step):
        below, above = (z + NZ - step) % NZ, (z + step) % NZ
        if step == 0:
            dy_in.wait_recv()
        else:
            dz_copy(below, 0, up).wait_recv()
        if step < 4:
            dz_copy(below, 0, up).start()
            dz_sent.append((below, 0, up))
        dc_copy(below).start()
        if 0 < step < 4:
            dz_copy(above, 1, down).wait_recv()
        if step < 3:
            dz_copy(above, 1, down).start()
            dz_sent.append((above, 1, down))
        if 0 < step < 4:
            dc_copy(above).start()

    load_a.wait()
    send(own_a, "right")
    send(own_a, "across")
    load_b.wait()
    send(own_b, "left")
    send(own_b, "right")
    send(own_a, "left")
    send(own_b, "across")
    load_delta.wait()
    dy_copy.start()
    load_cot.wait()
    cot_t[...] = cot[...].T
    gradients(own_a, own_b)
    delta_step(0)

    arrived(l_a)
    send(l_a, "right")
    send(l_a, "across")
    arrived(r_b)
    send(r_b, "left")
    send(r_b, "across")
    arrived(p_a)
    send(p_a, "left")
    gradients(l_a, r_b, p_a)
    delta_step(1)

    arrived(l_b)
    arrived(r_a)
    arrived(p_b)
    gradients(l_b, r_a, p_b)
    delta_step(2)

    arrived(pl_a)
    send(pl_a, "right")
    send(p_b, "right")
    arrived(ll_a)
    arrived(ll_b)
    gradients(ll_a, ll_b, pl_a)
    delta_step(3)

    arrived(pr_b)
    send(pr_b, "left")
    arrived(pr_a)
    arrived(pll_a)
    gradients(pr_a, pr_b, pll_a)
    delta_step(4)

    load_cache.wait()
    for origin in range(NZ):
        pltpu.make_async_remote_copy(
            src_ref=dbuf.at[origin, 1 - c], dst_ref=dbuf.at[origin, 1 - c],
            send_sem=dc_send.at[origin], recv_sem=dc_recv.at[origin],
            device_id=sibling, device_id_type=MESH,
        ).wait_recv()

    def rebuild(j, carry):
        rows = pl.ds(pl.multiple_of(j * BLOCK, BLOCK), BLOCK)
        change = dbuf[(j % 16) // 2, j % 2, j // 16]
        weight[rows, :] = (weight[rows, :].astype(F32) + change.astype(F32)).astype(BF16)
        return carry

    lax.fori_loop(0, 32, rebuild, 0)

    arrived(pl_b)
    arrived(pll_b)
    gradients(pl_b, pll_b)

    act[...] = jnp.zeros_like(act)

    def project(k, carry):
        first = pl.ds(pl.multiple_of(2 * k * HALF, HALF), HALF)
        second = pl.ds(pl.multiple_of((2 * k + 1) * HALF, HALF), HALF)
        terms = jnp.dot(tok[2 * k], weight[first, :], preferred_element_type=F32)
        terms += jnp.dot(tok[2 * k + 1], weight[second, :], preferred_element_type=F32)
        act[...] += terms
        return carry

    lax.fori_loop(0, 8, project, 0)

    def collected(rows):
        total = zloc[rows]
        for step in range(1, NZ):
            source = (z + step) % NZ
            pltpu.make_async_remote_copy(
                src_ref=zrcv.at[rows, source], dst_ref=zrcv.at[rows, source],
                send_sem=z_send.at[0], recv_sem=z_recv.at[rows, source],
                device_id={"z": source}, device_id_type=MESH,
            ).wait_recv()
            total = total + zrcv[rows, source].astype(F32)
        return total

    ysnd[...] = collected(1 - yl).astype(BF16)
    y_copy = pltpu.make_async_remote_copy(
        src_ref=ysnd, dst_ref=yrcv, send_sem=y_send, recv_sem=y_recv,
        device_id=beside, device_id_type=MESH,
    )
    y_copy.start()
    grad[...] = collected(yl)
    y_copy.wait_recv()
    grad[...] += yrcv[...].astype(F32)

    y_copy.wait_send()
    dy_copy.wait_send()
    for place, direction in sent:
        token_copy(place, direction).wait_send()
    for origin, lane, peer in dz_sent:
        dz_copy(origin, lane, peer).wait_send()

    def drain_delta(origin, carry):
        dc_copy(origin).wait_send()
        return carry

    def drain(place, carry):
        d2d_copy(place).wait_send()

        @pl.when(target(place)[1] != z)
        def _():
            z_copy(place).wait_send()

        return carry

    lax.fori_loop(0, NZ, drain_delta, 0)
    lax.fori_loop(0, 16, drain, 0)


def hadamard(length):
    first = lax.broadcasted_iota(jnp.int32, (length, length), 0)
    second = lax.broadcasted_iota(jnp.int32, (length, length), 1)
    common = jnp.bitwise_and(first, second)
    parity = jnp.zeros((length, length), jnp.int32)
    for place in range(length.bit_length() - 1):
        parity = parity + jnp.bitwise_and(jnp.right_shift(common, place), 1)
    signs = (1 - 2 * jnp.bitwise_and(parity, 1)).astype(F32)
    return signs / np.sqrt(np.float32(length))


def update(
    act_in, grad_t, sign_bits, master, moment, variance,
    act, new_master, new_moment, new_variance, scales,
    held, sem,
):
    fetch = pltpu.make_async_copy(act_in, held, sem.at[0])
    fetch.start()
    table = hadamard(BLOCK)
    fetch.wait()
    store = pltpu.make_async_copy(held, act, sem.at[1])
    store.start()
    for k in range(master.shape[1] // BLOCK):
        span = pl.ds(k * BLOCK, BLOCK)
        signs = (1 - 2 * sign_bits[:, span]).astype(F32)
        gradient = grad_t[span, :].T
        smoothed = jnp.dot(
            gradient * signs, table, precision=lax.Precision.HIGHEST, preferred_element_type=F32
        )
        scales[:, pl.ds(k, 1)] = jnp.max(jnp.abs(smoothed), axis=1, keepdims=True)
        restored = signs * jnp.dot(
            smoothed, table, precision=lax.Precision.HIGHEST, preferred_element_type=F32
        )
        first = 0.9 * moment[:, span] + 0.1 * restored
        second = 0.95 * variance[:, span] + 0.05 * restored * restored
        corrected = first / (1.0 - 0.9**10)
        spread = jnp.sqrt(second / (1.0 - 0.95**10)) + 1e-08
        old = master[:, span]
        new_moment[:, span] = first
        new_variance[:, span] = second
        new_master[:, span] = old - 0.01 * (corrected / spread + 0.1 * old)
    store.wait()


def body(tokens, cotangent, weight_cache, weight_delta, sign_bits, master, moment, variance):
    count, width = tokens.shape
    columns = cotangent.shape[1]
    inside = pl.BlockSpec(memory_space=pltpu.VMEM)
    outside = pl.BlockSpec(memory_space=pl.ANY)
    dma = pltpu.SemaphoreType.DMA
    piece = (columns, BLOCK)
    act, grad_t = pl.pallas_call(
        transport,
        out_shape=(
            jax.ShapeDtypeStruct((count, columns), F32),
            jax.ShapeDtypeStruct(piece, F32),
        ),
        in_specs=[outside] * 4,
        out_specs=(inside, inside),
        scratch_shapes=[
            pltpu.VMEM((16, count, HALF), BF16),
            pltpu.VMEM((count, columns), BF16),
            pltpu.VMEM((columns, count), BF16),
            pltpu.VMEM(weight_cache.shape, BF16),
            pltpu.VMEM((NZ, 2, 2, BLOCK, columns), BF16),
            pltpu.VMEM((16, 2, *piece), F32),
            pltpu.VMEM((16, *piece), F32),
            pltpu.VMEM((16, *piece), BF16),
            pltpu.VMEM((2, NZ, *piece), BF16),
            pltpu.VMEM((2, *piece), F32),
            pltpu.VMEM(piece, BF16),
            pltpu.VMEM(piece, BF16),
            dma((5,)), dma((3, 16)), dma((16,)), dma((16,)), dma((16,)), dma((16,)),
            dma((2, NZ)), dma, dma, dma((2,)), dma((2, NZ)), dma((NZ,)), dma((NZ,)), dma((NZ,)),
        ],
        compiler_params=pltpu.CompilerParams(
            collective_id=0, has_side_effects=True, vmem_limit_bytes=58 * 2**20
        ),
        name="transport",
    )(tokens, cotangent, weight_cache, weight_delta)
    small = jax.ShapeDtypeStruct(master.shape, F32)
    act, new_master, new_moment, new_variance, scales = pl.pallas_call(
        update,
        out_shape=(
            jax.ShapeDtypeStruct((count, columns), F32),
            small, small, small,
            jax.ShapeDtypeStruct((master.shape[0], columns // BLOCK), F32),
        ),
        in_specs=[outside] + [inside] * 5,
        out_specs=(outside, inside, inside, inside, inside),
        scratch_shapes=[pltpu.VMEM((count, columns), F32), dma((2,))],
        name="update",
    )(act, grad_t, sign_bits.reshape(1, columns), master, moment, variance)
    return act, new_master, new_moment, new_variance, scales


def solution(mesh):
    torus = Mesh(mesh.devices.reshape(NX, 2, 2, NZ, 2), OUTER + INNER)
    split = P(INNER, OUTER)
    return jax.shard_map(
        body, mesh=torus,
        in_specs=(split, split, P(None, OUTER), split, P(OUTER), split, split, split),
        out_specs=(split,) * 5,
        check_vma=False,
    )
```

```python
import functools

import jax
import jax.numpy as jnp
import numpy as np
from jax import lax
from jax.experimental import pallas as pl
from jax.experimental.pallas import tpu as pltpu
from jax.sharding import Mesh
from jax.sharding import PartitionSpec as P

BLOCK = 128
OUTER = ("x", "yh")
INNER = ("yl", "z", "c")
NX, NZ = 4, 8
HALF = 256
MESH = pl.DeviceIdType.MESH
F32, BF16 = jnp.float32, jnp.bfloat16


def transport(
    tokens, cotangent, cache, delta,
    act, grad,
    tok, cot, cot_t, weight, dbuf, gbuf, grcv, zsnd, zmid, zrcv, zloc, ysnd, yrcv,
    load_sem, tok_send, tok_recv, d2d_send, d2d_recv, z_send, m_recv, z_recv, y_send, y_recv,
    dy_sem, dz_send, dz_recv, dc_send, dc_recv,
):
    x, yh, yl = lax.axis_index("x"), lax.axis_index("yh"), lax.axis_index("yl")
    z, c = lax.axis_index("z"), lax.axis_index("c")
    right, left = {"x": (x + 1) % NX}, {"x": (x + 3) % NX}
    across, beside, sibling = {"yh": 1 - yh}, {"yl": 1 - yl}, {"c": 1 - c}
    up, down = {"z": (z + 1) % NZ}, {"z": (z + 7) % NZ}

    def slot(dx, dy, half):
        row = yh if dy == 0 else 1 - yh
        return 4 * ((x + dx) % NX) + 2 * row + half

    own_a, own_b = slot(0, 0, 0), slot(0, 0, 1)
    l_a, l_b, r_a, r_b = slot(3, 0, 0), slot(3, 0, 1), slot(1, 0, 0), slot(1, 0, 1)
    ll_a, ll_b = slot(2, 0, 0), slot(2, 0, 1)
    p_a, p_b = slot(0, 1, 0), slot(0, 1, 1)
    pl_a, pl_b, pr_a, pr_b = slot(3, 1, 0), slot(3, 1, 1), slot(1, 1, 0), slot(1, 1, 1)
    pll_a, pll_b = slot(2, 1, 0), slot(2, 1, 1)

    load_a = pltpu.make_async_copy(tokens.at[:, pl.ds(0, HALF)], tok.at[own_a], load_sem.at[0])
    load_b = pltpu.make_async_copy(tokens.at[:, pl.ds(HALF, HALF)], tok.at[own_b], load_sem.at[1])
    load_cot = pltpu.make_async_copy(cotangent, cot, load_sem.at[2])
    load_delta = pltpu.make_async_copy(delta, dbuf.at[z, c, yl], load_sem.at[3])
    load_cache = pltpu.make_async_copy(cache, weight, load_sem.at[4])
    for copy in (load_delta, load_a, load_b, load_cot, load_cache):
        copy.start()

    barrier = pltpu.get_barrier_semaphore()
    peers = [right, left, across, beside, sibling]
    peers += [{"z": (z + step) % NZ} for step in range(1, NZ)]
    for peer in peers:
        pl.semaphore_signal(barrier, inc=1, device_id=peer, device_id_type=MESH)
    pl.semaphore_wait(barrier, len(peers))

    way = {"right": (0, right), "left": (1, left), "across": (2, across)}

    def token_copy(place, direction):
        lane, peer = way[direction]
        return pltpu.make_async_remote_copy(
            src_ref=tok.at[place], dst_ref=tok.at[place],
            send_sem=tok_send.at[lane, place], recv_sem=tok_recv.at[place],
            device_id=peer, device_id_type=MESH,
        )

    sent = []

    def send(place, direction):
        token_copy(place, direction).start()
        sent.append((place, direction))

    def arrived(place):
        token_copy(place, "right").wait_recv()

    def d2d_copy(place):
        return pltpu.make_async_remote_copy(
            src_ref=gbuf.at[place, 1 - c], dst_ref=grcv.at[place],
            send_sem=d2d_send.at[place], recv_sem=d2d_recv.at[place],
            device_id=sibling, device_id_type=MESH,
        )

    def target(place):
        block = place // 2
        return block // 4, 2 * (block % 4) + place % 2

    def offset(place):
        return (z - target(place)[1] + NZ) % NZ

    def mid_copy(place):
        away, depth = offset(place), target(place)[1]
        far = jnp.where(away == 4, 1, 0)
        side = jnp.where(away == 3, 2, jnp.where(away == 5, 6, 2 + 4 * (place % 2)))
        return pltpu.make_async_remote_copy(
            src_ref=zsnd.at[place], dst_ref=zmid.at[place, far],
            send_sem=z_send.at[place], recv_sem=m_recv.at[place, far],
            device_id={"z": (depth + side) % NZ}, device_id_type=MESH,
        )

    def z_copy(place):
        rows, depth = target(place)
        away = offset(place)
        entry = jnp.where(away < 3, away - 1, away - 4)
        return pltpu.make_async_remote_copy(
            src_ref=zsnd.at[place], dst_ref=zrcv.at[rows, entry],
            send_sem=z_send.at[place], recv_sem=z_recv.at[rows, entry],
            device_id={"z": depth}, device_id_type=MESH,
        )

    def pick(places, i):
        value = places[0]
        for k in range(1, len(places)):
            value = jnp.where(i == k, places[k], value)
        return value

    def gradients(*places):
        def product(i, carry):
            place = pick(places, i)
            terms = jnp.dot(cot_t[...], tok[place], preferred_element_type=F32)
            gbuf[place, 0] = terms[:, :BLOCK]
            gbuf[place, 1] = terms[:, BLOCK:]
            d2d_copy(place).start()
            return carry

        def merge(i, carry):
            place = pick(places, i)
            d2d_copy(place).wait_recv()
            total = gbuf[place, c] + grcv[place]
            away = offset(place)
            zsnd[place] = total.astype(BF16)

            @pl.when((away == 1) | (away == 7))
            def _():
                z_copy(place).start()

            @pl.when((away >= 3) & (away <= 5))
            def _():
                mid_copy(place).start()

            @pl.when((away == 2) | (away == 6))
            def _():
                gbuf[place, c] = total

            @pl.when(away == 0)
            def _():
                zloc[target(place)[0]] = total

            return carry

        lax.fori_loop(0, len(places), product, 0)
        lax.fori_loop(0, len(places), merge, 0)

    def relays(*places):
        def relay(i, carry):
            place = pick(places, i)
            away = offset(place)

            def inflow(far):
                return pltpu.make_async_remote_copy(
                    src_ref=zmid.at[place, far], dst_ref=zmid.at[place, far],
                    send_sem=z_send.at[place], recv_sem=m_recv.at[place, far],
                    device_id=up, device_id_type=MESH,
                )

            @pl.when(away == 2 + 4 * (place % 2))
            def _():
                inflow(1).wait_recv()
                gbuf[place, c] += zmid[place, 1].astype(F32)

            @pl.when((away == 2) | (away == 6))
            def _():
                inflow(0).wait_recv()
                zsnd[place] = (gbuf[place, c] + zmid[place, 0].astype(F32)).astype(BF16)
                z_copy(place).start()

            return carry

        lax.fori_loop(0, len(places), relay, 0)

    def dz_copy(origin, lane, peer):
        return pltpu.make_async_remote_copy(
            src_ref=dbuf.at[origin, c], dst_ref=dbuf.at[origin, c],
            send_sem=dz_send.at[lane, origin], recv_sem=dz_recv.at[origin],
            device_id=peer, device_id_type=MESH,
        )

    def dc_copy(origin):
        return pltpu.make_async_remote_copy(
            src_ref=dbuf.at[origin, c], dst_ref=dbuf.at[origin, c],
            send_sem=dc_send.at[origin], recv_sem=dc_recv.at[origin],
            device_id=sibling, device_id_type=MESH,
        )

    dy_copy = pltpu.make_async_remote_copy(
        src_ref=dbuf.at[z, c, yl], dst_ref=dbuf.at[z, c, yl],
        send_sem=dy_sem.at[0], recv_sem=dy_sem.at[1],
        device_id=beside, device_id_type=MESH,
    )
    dy_in = pltpu.make_async_remote_copy(
        src_ref=dbuf.at[z, c, 1 - yl], dst_ref=dbuf.at[z, c, 1 - yl],
        send_sem=dy_sem.at[0], recv_sem=dy_sem.at[1],
        device_id=beside, device_id_type=MESH,
    )
    dz_sent = []

    def delta_step(step):
        below, above = (z + NZ - step) % NZ, (z + step) % NZ
        if step == 0:
            dy_in.wait_recv()
        else:
            dz_copy(below, 0, up).wait_recv()
        if step < 4:
            dz_copy(below, 0, up).start()
            dz_sent.append((below, 0, up))
        dc_copy(below).start()
        if 0 < step < 4:
            dz_copy(above, 1, down).wait_recv()
        if step < 3:
            dz_copy(above, 1, down).start()
            dz_sent.append((above, 1, down))
        if 0 < step < 4:
            dc_copy(above).start()

    load_delta.wait()
    dy_copy.start()
    load_a.wait()
    send(own_a, "right")
    send(own_a, "across")
    load_b.wait()
    send(own_b, "left")
    send(own_b, "right")
    send(own_a, "left")
    send(own_b, "across")
    load_cot.wait()
    cot_t[...] = cot[...].T
    gradients(own_a, own_b)
    delta_step(0)

    arrived(l_a)
    send(l_a, "right")
    send(l_a, "across")
    arrived(r_b)
    send(r_b, "left")
    send(r_b, "across")
    arrived(p_a)
    send(p_a, "left")
    delta_step(1)
    gradients(l_a, r_b, p_a)
    relays(own_a, own_b)

    arrived(l_b)
    arrived(r_a)
    arrived(p_b)
    delta_step(2)
    gradients(l_b, r_a, p_b)
    relays(l_a, r_b, p_a)

    arrived(pl_a)
    send(pl_a, "right")
    send(p_b, "right")
    arrived(ll_a)
    arrived(ll_b)
    delta_step(3)
    gradients(ll_a, ll_b, pl_a)
    relays(l_b, r_a, p_b)

    arrived(pr_b)
    send(pr_b, "left")
    arrived(pr_a)
    arrived(pll_a)
    delta_step(4)
    gradients(pr_a, pr_b, pll_a)
    relays(ll_a, ll_b, pl_a)

    load_cache.wait()
    for origin in range(NZ):
        pltpu.make_async_remote_copy(
            src_ref=dbuf.at[origin, 1 - c], dst_ref=dbuf.at[origin, 1 - c],
            send_sem=dc_send.at[origin], recv_sem=dc_recv.at[origin],
            device_id=sibling, device_id_type=MESH,
        ).wait_recv()

    def rebuild(j, carry):
        rows = pl.ds(pl.multiple_of(j * BLOCK, BLOCK), BLOCK)
        change = dbuf[(j % 16) // 2, j % 2, j // 16]
        weight[rows, :] = (weight[rows, :].astype(F32) + change.astype(F32)).astype(BF16)
        return carry

    lax.fori_loop(0, 32, rebuild, 0)
    act[...] = jnp.zeros_like(act)

    def project(*firsts):
        def add(i, carry):
            place = pick(firsts, i)
            first = pl.ds(pl.multiple_of(place * HALF, HALF), HALF)
            second = pl.ds(pl.multiple_of((place + 1) * HALF, HALF), HALF)
            terms = jnp.dot(tok[place], weight[first, :], preferred_element_type=F32)
            terms += jnp.dot(tok[place + 1], weight[second, :], preferred_element_type=F32)
            act[...] += terms
            return carry

        lax.fori_loop(0, len(firsts), add, 0)

    project(own_a, l_a, r_a, p_a)
    relays(pr_a, pr_b, pll_a)

    arrived(pl_b)
    arrived(pll_b)
    gradients(pl_b, pll_b)
    project(ll_a, pr_a)
    relays(pl_b, pll_b)
    project(pl_a, pll_a)

    def collected(rows):
        total = zloc[rows]
        for entry in range(4):
            pltpu.make_async_remote_copy(
                src_ref=zrcv.at[rows, entry], dst_ref=zrcv.at[rows, entry],
                send_sem=z_send.at[0], recv_sem=z_recv.at[rows, entry],
                device_id=up, device_id_type=MESH,
            ).wait_recv()
            total = total + zrcv[rows, entry].astype(F32)
        return total

    ysnd[...] = collected(1 - yl).astype(BF16)
    y_copy = pltpu.make_async_remote_copy(
        src_ref=ysnd, dst_ref=yrcv, send_sem=y_send, recv_sem=y_recv,
        device_id=beside, device_id_type=MESH,
    )
    y_copy.start()
    grad[...] = collected(yl)
    y_copy.wait_recv()
    grad[...] += yrcv[...].astype(F32)

    y_copy.wait_send()
    dy_copy.wait_send()
    for place, direction in sent:
        token_copy(place, direction).wait_send()
    for origin, lane, peer in dz_sent:
        dz_copy(origin, lane, peer).wait_send()

    def drain_delta(origin, carry):
        dc_copy(origin).wait_send()
        return carry

    def drain(place, carry):
        d2d_copy(place).wait_send()

        @pl.when(offset(place) != 0)
        def _():
            pltpu.make_async_remote_copy(
                src_ref=zsnd.at[place], dst_ref=zmid.at[place, 0],
                send_sem=z_send.at[place], recv_sem=m_recv.at[place, 0],
                device_id=up, device_id_type=MESH,
            ).wait_send()

        return carry

    lax.fori_loop(0, NZ, drain_delta, 0)
    lax.fori_loop(0, 16, drain, 0)


def hadamard(length):
    first = lax.broadcasted_iota(jnp.int32, (length, length), 0)
    second = lax.broadcasted_iota(jnp.int32, (length, length), 1)
    common = jnp.bitwise_and(first, second)
    parity = jnp.zeros((length, length), jnp.int32)
    for place in range(length.bit_length() - 1):
        parity = parity + jnp.bitwise_and(jnp.right_shift(common, place), 1)
    signs = (1 - 2 * jnp.bitwise_and(parity, 1)).astype(F32)
    return signs / np.sqrt(np.float32(length))


def update(
    act_in, grad_t, sign_bits, master, moment, variance,
    act, new_master, new_moment, new_variance, scales,
    held, sem,
):
    fetch = pltpu.make_async_copy(act_in, held, sem.at[0])
    fetch.start()
    table = hadamard(BLOCK)
    fetch.wait()
    store = pltpu.make_async_copy(held, act, sem.at[1])
    store.start()
    for k in range(master.shape[1] // BLOCK):
        span = pl.ds(k * BLOCK, BLOCK)
        signs = (1 - 2 * sign_bits[:, span]).astype(F32)
        gradient = grad_t[span, :].T
        smoothed = jnp.dot(
            gradient * signs, table, precision=lax.Precision.HIGHEST, preferred_element_type=F32
        )
        scales[pl.ds(k, 1), :] = jnp.max(jnp.abs(smoothed.T), axis=0, keepdims=True)
        restored = signs * jnp.dot(
            smoothed, table, precision=lax.Precision.HIGHEST, preferred_element_type=F32
        )
        first = 0.9 * moment[:, span] + 0.1 * restored
        second = 0.95 * variance[:, span] + 0.05 * restored * restored
        corrected = first / (1.0 - 0.9**10)
        spread = jnp.sqrt(second / (1.0 - 0.95**10)) + 1e-08
        old = master[:, span]
        new_moment[:, span] = first
        new_variance[:, span] = second
        new_master[:, span] = old - 0.01 * (corrected / spread + 0.1 * old)
    store.wait()


def body(tokens, cotangent, weight_cache, weight_delta, sign_bits, master, moment, variance):
    count, width = tokens.shape
    columns = cotangent.shape[1]
    inside = pl.BlockSpec(memory_space=pltpu.VMEM)
    outside = pl.BlockSpec(memory_space=pl.ANY)
    dma = pltpu.SemaphoreType.DMA
    piece = (columns, BLOCK)
    act, grad_t = pl.pallas_call(
        transport,
        out_shape=(
            jax.ShapeDtypeStruct((count, columns), F32),
            jax.ShapeDtypeStruct(piece, F32),
        ),
        in_specs=[outside] * 4,
        out_specs=(inside, inside),
        scratch_shapes=[
            pltpu.VMEM((16, count, HALF), BF16),
            pltpu.VMEM((count, columns), BF16),
            pltpu.VMEM((columns, count), BF16),
            pltpu.VMEM(weight_cache.shape, BF16),
            pltpu.VMEM((NZ, 2, 2, BLOCK, columns), BF16),
            pltpu.VMEM((16, 2, *piece), F32),
            pltpu.VMEM((16, *piece), F32),
            pltpu.VMEM((16, *piece), BF16),
            pltpu.VMEM((16, 2, *piece), BF16),
            pltpu.VMEM((2, 4, *piece), BF16),
            pltpu.VMEM((2, *piece), F32),
            pltpu.VMEM(piece, BF16),
            pltpu.VMEM(piece, BF16),
            dma((5,)), dma((3, 16)), dma((16,)), dma((16,)), dma((16,)), dma((16,)),
            dma((16, 2)), dma((2, 4)), dma, dma, dma((2,)), dma((2, NZ)), dma((NZ,)), dma((NZ,)), dma((NZ,)),
        ],
        compiler_params=pltpu.CompilerParams(
            collective_id=0, has_side_effects=True, vmem_limit_bytes=58 * 2**20
        ),
        name="transport",
    )(tokens, cotangent, weight_cache, weight_delta)
    small = jax.ShapeDtypeStruct(master.shape, F32)
    act, new_master, new_moment, new_variance, scales = pl.pallas_call(
        update,
        out_shape=(
            jax.ShapeDtypeStruct((count, columns), F32),
            small, small, small,
            jax.ShapeDtypeStruct((columns // BLOCK, master.shape[0]), F32),
        ),
        in_specs=[outside] + [inside] * 5,
        out_specs=(outside, inside, inside, inside, inside),
        scratch_shapes=[pltpu.VMEM((count, columns), F32), dma((2,))],
        name="update",
    )(act, grad_t, sign_bits.reshape(1, columns), master, moment, variance)
    return act, new_master, new_moment, new_variance, scales.T


def solution(mesh):
    torus = Mesh(mesh.devices.reshape(NX, 2, 2, NZ, 2), OUTER + INNER)
    split = P(INNER, OUTER)
    return jax.shard_map(
        body, mesh=torus,
        in_specs=(split, split, P(None, OUTER), split, P(OUTER), split, split, split),
        out_specs=(split,) * 5,
        check_vma=False,
    )
```

```python
import functools

import jax
import jax.numpy as jnp
import numpy as np
from jax import lax
from jax.experimental import pallas as pl
from jax.experimental.pallas import tpu as pltpu
from jax.sharding import Mesh
from jax.sharding import PartitionSpec as P

BLOCK = 128
OUTER = ("x", "yh")
INNER = ("yl", "z", "c")
NX, NZ = 4, 8
HALF = 256
MESH = pl.DeviceIdType.MESH
F32, BF16 = jnp.float32, jnp.bfloat16


def transport(
    tokens, cotangent, cache, delta,
    act_out, grad_out,
    act, grad, tok, cot, cot_t, weight, dbuf, gbuf, grcv, zsnd, zmid, zrcv, zloc, ysnd, yrcv,
    load_sem, tok_send, tok_recv, d2d_send, d2d_recv, z_send, m_recv, z_recv, y_send, y_recv,
    dy_sem, dz_send, dz_recv, dc_send, dc_recv,
):
    x, yh, yl = lax.axis_index("x"), lax.axis_index("yh"), lax.axis_index("yl")
    z, c = lax.axis_index("z"), lax.axis_index("c")
    right, left = {"x": (x + 1) % NX}, {"x": (x + 3) % NX}
    across, beside, sibling = {"yh": 1 - yh}, {"yl": 1 - yl}, {"c": 1 - c}
    up, down = {"z": (z + 1) % NZ}, {"z": (z + 7) % NZ}

    def slot(dx, dy, half):
        row = yh if dy == 0 else 1 - yh
        return 4 * ((x + dx) % NX) + 2 * row + half

    own_a, own_b = slot(0, 0, 0), slot(0, 0, 1)
    l_a, l_b, r_a, r_b = slot(3, 0, 0), slot(3, 0, 1), slot(1, 0, 0), slot(1, 0, 1)
    ll_a, ll_b = slot(2, 0, 0), slot(2, 0, 1)
    p_a, p_b = slot(0, 1, 0), slot(0, 1, 1)
    pl_a, pl_b, pr_a, pr_b = slot(3, 1, 0), slot(3, 1, 1), slot(1, 1, 0), slot(1, 1, 1)
    pll_a, pll_b = slot(2, 1, 0), slot(2, 1, 1)

    loads = [
        pltpu.make_async_copy(
            tokens.at[:, pl.ds(BLOCK * k, BLOCK)], tok.at[2 * own_a + k], load_sem.at[k]
        )
        for k in range(4)
    ]
    load_cot = pltpu.make_async_copy(cotangent, cot, load_sem.at[4])
    load_delta = pltpu.make_async_copy(delta, dbuf.at[z, c, yl], load_sem.at[5])
    load_cache = pltpu.make_async_copy(cache, weight, load_sem.at[6])
    for copy in (load_delta, *loads, load_cot, load_cache):
        copy.start()

    barrier = pltpu.get_barrier_semaphore()
    peers = [right, left, across, beside, sibling]
    peers += [{"z": (z + step) % NZ} for step in range(1, NZ)]
    for peer in peers:
        pl.semaphore_signal(barrier, inc=1, device_id=peer, device_id_type=MESH)
    pl.semaphore_wait(barrier, len(peers))

    way = {"right": (0, right), "left": (1, left), "across": (2, across)}

    def token_copy(place, direction, part=None):
        lane, peer = way[direction]
        first = 2 * place if part is None else 2 * place + part
        piece = pl.ds(first, 2 if part is None else 1)
        return pltpu.make_async_remote_copy(
            src_ref=tok.at[piece], dst_ref=tok.at[piece],
            send_sem=tok_send.at[lane], recv_sem=tok_recv.at[first],
            device_id=peer, device_id_type=MESH,
        )

    def send(place, direction, part=None):
        token_copy(place, direction, part).start()

    def arrived(place, part=None):
        token_copy(place, "right", part).wait_recv()

    def d2d_copy(place):
        return pltpu.make_async_remote_copy(
            src_ref=gbuf.at[place, 1 - c], dst_ref=grcv.at[place],
            send_sem=d2d_send, recv_sem=d2d_recv.at[place],
            device_id=sibling, device_id_type=MESH,
        )

    def target(place):
        block = place // 2
        return block // 4, 2 * (block % 4) + place % 2

    def offset(place):
        return (z - target(place)[1] + NZ) % NZ

    def mid_copy(place):
        away, depth = offset(place), target(place)[1]
        far = jnp.where(away == 4, 1, 0)
        side = jnp.where(away == 3, 2, jnp.where(away == 5, 6, 2 + 4 * (place % 2)))
        return pltpu.make_async_remote_copy(
            src_ref=zsnd.at[place], dst_ref=zmid.at[place, far],
            send_sem=z_send, recv_sem=m_recv.at[place, far],
            device_id={"z": (depth + side) % NZ}, device_id_type=MESH,
        )

    def z_copy(place):
        rows, depth = target(place)
        away = offset(place)
        entry = jnp.where(away < 3, away - 1, away - 4)
        return pltpu.make_async_remote_copy(
            src_ref=zsnd.at[place], dst_ref=zrcv.at[rows, entry],
            send_sem=z_send, recv_sem=z_recv.at[rows, entry],
            device_id={"z": depth}, device_id_type=MESH,
        )

    def pick(places, i):
        value = places[0]
        for k in range(1, len(places)):
            value = jnp.where(i == k, places[k], value)
        return value

    def merge(place):
        d2d_copy(place).wait_recv()
        total = gbuf[place, c] + grcv[place]
        away = offset(place)
        zsnd[place] = total.astype(BF16)

        @pl.when((away == 1) | (away == 7))
        def _():
            z_copy(place).start()

        @pl.when((away >= 3) & (away <= 5))
        def _():
            mid_copy(place).start()

        @pl.when((away == 2) | (away == 6))
        def _():
            gbuf[place, c] = total

        @pl.when(away == 0)
        def _():
            zloc[target(place)[0]] = total

    def gradients(*places):
        def product(i, carry):
            place = pick(places, i)
            both = jnp.concatenate([tok[2 * place], tok[2 * place + 1]], axis=1)
            terms = jnp.dot(cot_t[...], both, preferred_element_type=F32)
            gbuf[place, 0] = terms[:, :BLOCK]
            gbuf[place, 1] = terms[:, BLOCK:]
            d2d_copy(place).start()
            return carry

        def finish(i, carry):
            merge(pick(places, i))
            return carry

        lax.fori_loop(0, len(places), product, 0)
        lax.fori_loop(0, len(places), finish, 0)

    def quarters(part, *places):
        def product(i, carry):
            place = pick(places, i)
            terms = jnp.dot(cot_t[...], tok[2 * place + part], preferred_element_type=F32)
            gbuf[place, part] = terms

            @pl.when(c != part)
            def _():
                d2d_copy(place).start()

            return carry

        def finish(i, carry):
            @pl.when(c == part)
            def _():
                merge(pick(places, i))

            return carry

        lax.fori_loop(0, len(places), product, 0)
        lax.fori_loop(0, len(places), finish, 0)

    def relays(*places):
        def relay(i, carry):
            place = pick(places, i)
            away = offset(place)

            def inflow(far):
                return pltpu.make_async_remote_copy(
                    src_ref=zmid.at[place, far], dst_ref=zmid.at[place, far],
                    send_sem=z_send, recv_sem=m_recv.at[place, far],
                    device_id=up, device_id_type=MESH,
                )

            @pl.when(away == 2 + 4 * (place % 2))
            def _():
                inflow(1).wait_recv()
                gbuf[place, c] += zmid[place, 1].astype(F32)

            @pl.when((away == 2) | (away == 6))
            def _():
                inflow(0).wait_recv()
                zsnd[place] = (gbuf[place, c] + zmid[place, 0].astype(F32)).astype(BF16)
                z_copy(place).start()

            return carry

        lax.fori_loop(0, len(places), relay, 0)

    def dz_copy(origin, peer):
        return pltpu.make_async_remote_copy(
            src_ref=dbuf.at[origin, c], dst_ref=dbuf.at[origin, c],
            send_sem=dz_send, recv_sem=dz_recv.at[origin],
            device_id=peer, device_id_type=MESH,
        )

    def dc_copy(origin):
        return pltpu.make_async_remote_copy(
            src_ref=dbuf.at[origin, c], dst_ref=dbuf.at[origin, c],
            send_sem=dc_send, recv_sem=dc_recv,
            device_id=sibling, device_id_type=MESH,
        )

    dy_copy = pltpu.make_async_remote_copy(
        src_ref=dbuf.at[z, c, yl], dst_ref=dbuf.at[z, c, yl],
        send_sem=dy_sem.at[0], recv_sem=dy_sem.at[1],
        device_id=beside, device_id_type=MESH,
    )
    dy_in = pltpu.make_async_remote_copy(
        src_ref=dbuf.at[z, c, 1 - yl], dst_ref=dbuf.at[z, c, 1 - yl],
        send_sem=dy_sem.at[0], recv_sem=dy_sem.at[1],
        device_id=beside, device_id_type=MESH,
    )

    def delta_step(step):
        below, above = (z + NZ - step) % NZ, (z + step) % NZ
        if step == 0:
            dy_in.wait_recv()
        else:
            dz_copy(below, up).wait_recv()
        if step < 4:
            dz_copy(below, up).start()
        dc_copy(below).start()
        if 0 < step < 4:
            dz_copy(above, down).wait_recv()
        if step < 3:
            dz_copy(above, down).start()
        if 0 < step < 4:
            dc_copy(above).start()

    def rebuild(j, carry):
        rows = pl.ds(pl.multiple_of(j * BLOCK, BLOCK), BLOCK)
        change = dbuf[(j % 16) // 2, j % 2, j // 16]
        weight[rows, :] = (weight[rows, :].astype(F32) + change.astype(F32)).astype(BF16)
        return carry

    def project(*firsts):
        def add(i, carry):
            first = pick(firsts, i)
            rows = pl.ds(pl.multiple_of(first * HALF, HALF), 2 * HALF)
            block = jnp.concatenate([tok[2 * first + k] for k in range(4)], axis=1)
            act[...] += jnp.dot(block, weight[rows, :], preferred_element_type=F32)
            return carry

        lax.fori_loop(0, len(firsts), add, 0)

    load_delta.wait()
    dy_copy.start()
    loads[0].wait()
    loads[1].wait()
    send(own_a, "right")
    send(own_a, "across")
    loads[2].wait()
    loads[3].wait()
    send(own_b, "left")
    send(own_b, "right")
    send(own_a, "left")
    load_cot.wait()
    cot_t[...] = cot[...].T
    gradients(own_a, own_b)
    delta_step(0)
    act[...] = jnp.zeros_like(act)

    arrived(l_a)
    send(l_a, "right")
    send(l_a, "across")
    send(own_b, "across")
    arrived(r_b)
    send(r_b, "left")
    send(r_b, "across", 0)
    send(r_b, "across", 1)
    arrived(p_a)
    send(p_a, "left")
    delta_step(1)
    gradients(l_a, r_b, p_a)
    relays(own_a, own_b)

    arrived(l_b)
    arrived(r_a)
    arrived(pl_a)
    send(pl_a, "right")
    delta_step(2)
    gradients(l_b, r_a, pl_a)
    relays(l_a, r_b, p_a)

    arrived(ll_a)
    arrived(ll_b)
    arrived(p_b)
    send(p_b, "right", 0)
    send(p_b, "right", 1)
    delta_step(3)
    gradients(ll_a, ll_b, p_b)
    relays(l_b, r_a, pl_a)

    arrived(pr_b, 0)
    send(pr_b, "left", 0)
    arrived(pr_b, 1)
    send(pr_b, "left", 1)
    relays(ll_a, ll_b, p_b)
    delta_step(4)
    arrived(pr_a)
    arrived(pll_a)
    gradients(pr_a, pr_b, pll_a)

    arrived(pl_b, 0)
    arrived(pll_b, 0)
    quarters(0, pl_b, pll_b)
    load_cache.wait()
    pltpu.make_async_remote_copy(
        src_ref=dbuf.at[:, 1 - c], dst_ref=dbuf.at[:, 1 - c],
        send_sem=dc_send, recv_sem=dc_recv,
        device_id=sibling, device_id_type=MESH,
    ).wait_recv()
    lax.fori_loop(0, 32, rebuild, 0)
    arrived(pl_b, 1)
    arrived(pll_b, 1)
    quarters(1, pl_b, pll_b)
    relays(pr_a, pr_b, pll_a)
    project(own_a, l_a, r_a)
    relays(pl_b, pll_b)
    project(p_a, ll_a, pr_a, pl_a, pll_a)
    store_act = pltpu.make_async_copy(act, act_out, load_sem.at[7])
    store_act.start()

    def collected(rows):
        total = zloc[rows]
        for entry in range(4):
            pltpu.make_async_remote_copy(
                src_ref=zrcv.at[rows, entry], dst_ref=zrcv.at[rows, entry],
                send_sem=z_send, recv_sem=z_recv.at[rows, entry],
                device_id=up, device_id_type=MESH,
            ).wait_recv()
            total = total + zrcv[rows, entry].astype(F32)
        return total

    ysnd[...] = collected(1 - yl).astype(BF16)
    y_copy = pltpu.make_async_remote_copy(
        src_ref=ysnd, dst_ref=yrcv, send_sem=y_send, recv_sem=y_recv,
        device_id=beside, device_id_type=MESH,
    )
    y_copy.start()
    grad[...] = collected(yl)
    y_copy.wait_recv()
    grad[...] += yrcv[...].astype(F32)
    store_grad = pltpu.make_async_copy(grad, grad_out, load_sem.at[8])
    store_grad.start()

    y_copy.wait_send()
    dy_copy.wait_send()
    def sent(block, sem):
        pltpu.make_async_remote_copy(
            src_ref=block, dst_ref=block, send_sem=sem, recv_sem=y_recv,
            device_id=beside, device_id_type=MESH,
        ).wait_send()

    sent(tok.at[pl.ds(0, 10)], tok_send.at[0])
    sent(tok.at[pl.ds(0, 10)], tok_send.at[1])
    sent(tok.at[pl.ds(0, 8)], tok_send.at[2])
    sent(dbuf.at[pl.ds(0, 7), c], dz_send)
    sent(dbuf.at[:, c], dc_send)
    sent(grcv, d2d_send)
    sent(zsnd.at[pl.ds(0, 14)], z_send)
    store_act.wait()
    store_grad.wait()


def hadamard(length):
    first = lax.broadcasted_iota(jnp.int32, (length, length), 0)
    second = lax.broadcasted_iota(jnp.int32, (length, length), 1)
    common = jnp.bitwise_and(first, second)
    parity = jnp.zeros((length, length), jnp.int32)
    for place in range(length.bit_length() - 1):
        parity = parity + jnp.bitwise_and(jnp.right_shift(common, place), 1)
    signs = (1 - 2 * jnp.bitwise_and(parity, 1)).astype(F32)
    return signs / np.sqrt(np.float32(length))


def update(
    act_in, grad_t, sign_bits, master, moment, variance,
    act, new_master, new_moment, new_variance, scales,
    held, grad, bits, old, out, peaks, sem_in, sem_held, sem_out,
):
    pieces = 4
    rows = held.shape[0] // pieces
    spans = [pl.ds(k * rows, rows) for k in range(pieces)]
    fetches = [
        pltpu.make_async_copy(source, target, sem_in.at[k])
        for k, (source, target) in enumerate((
            (grad_t, grad), (sign_bits, bits), (master, old.at[0]), (moment, old.at[1]), (variance, old.at[2])
        ))
    ]
    moves = [
        (
            pltpu.make_async_copy(act_in.at[span], held.at[span], sem_held.at[0, k]),
            pltpu.make_async_copy(held.at[span], act.at[span], sem_held.at[1, k]),
        )
        for k, span in enumerate(spans)
    ]
    for copy in fetches:
        copy.start()
    for fetch, _ in moves:
        fetch.start()
    table = hadamard(BLOCK)
    for copy in fetches:
        copy.wait()
    for fetch, store in moves:
        fetch.wait()
        store.start()
    for k in range(old.shape[2] // BLOCK):
        span = pl.ds(k * BLOCK, BLOCK)
        signs = (1 - 2 * bits[:, span]).astype(F32)
        gradient = grad[span, :].T
        smoothed = jnp.dot(
            gradient * signs, table, precision=lax.Precision.HIGHEST, preferred_element_type=F32
        )
        peaks[pl.ds(k, 1), :] = jnp.max(jnp.abs(smoothed.T), axis=0, keepdims=True)
        restored = signs * jnp.dot(
            smoothed, table, precision=lax.Precision.HIGHEST, preferred_element_type=F32
        )
        first = 0.9 * old[1, :, span] + 0.1 * restored
        second = 0.95 * old[2, :, span] + 0.05 * restored * restored
        corrected = first / (1.0 - 0.9**10)
        spread = jnp.sqrt(second / (1.0 - 0.95**10)) + 1e-08
        weight = old[0, :, span]
        out[0, :, span] = weight - 0.01 * (corrected / spread + 0.1 * weight)
        out[1, :, span] = first
        out[2, :, span] = second
    stores = [
        pltpu.make_async_copy(out.at[k], target, sem_out.at[k])
        for k, target in enumerate((new_master, new_moment, new_variance))
    ]
    stores.append(pltpu.make_async_copy(peaks, scales, sem_out.at[3]))
    for copy in stores:
        copy.start()
    for _, store in moves:
        store.wait()
    for copy in stores:
        copy.wait()


def body(tokens, cotangent, weight_cache, weight_delta, sign_bits, master, moment, variance):
    count, width = tokens.shape
    columns = cotangent.shape[1]
    inside = pl.BlockSpec(memory_space=pltpu.VMEM)
    outside = pl.BlockSpec(memory_space=pltpu.HBM)
    dma = pltpu.SemaphoreType.DMA
    piece = (columns, BLOCK)
    act, grad_t = pl.pallas_call(
        transport,
        out_shape=(
            jax.ShapeDtypeStruct((count, columns), F32),
            jax.ShapeDtypeStruct(piece, F32),
        ),
        in_specs=[outside] * 4,
        out_specs=(outside, outside),
        scratch_shapes=[
            pltpu.VMEM((count, columns), F32),
            pltpu.VMEM(piece, F32),
            pltpu.VMEM((32, count, BLOCK), BF16),
            pltpu.VMEM((count, columns), BF16),
            pltpu.VMEM((columns, count), BF16),
            pltpu.VMEM(weight_cache.shape, BF16),
            pltpu.VMEM((NZ, 2, 2, BLOCK, columns), BF16),
            pltpu.VMEM((16, 2, *piece), F32),
            pltpu.VMEM((16, *piece), F32),
            pltpu.VMEM((16, *piece), BF16),
            pltpu.VMEM((16, 2, *piece), BF16),
            pltpu.VMEM((2, 4, *piece), BF16),
            pltpu.VMEM((2, *piece), F32),
            pltpu.VMEM(piece, BF16),
            pltpu.VMEM(piece, BF16),
            dma((9,)), dma((3,)), dma((32,)), dma, dma((16,)), dma,
            dma((16, 2)), dma((2, 4)), dma, dma, dma((2,)), dma, dma((NZ,)), dma, dma,
        ],
        compiler_params=pltpu.CompilerParams(
            collective_id=0, has_side_effects=True, vmem_limit_bytes=58 * 2**20
        ),
        name="transport",
    )(tokens, cotangent, weight_cache, weight_delta)
    small = jax.ShapeDtypeStruct(master.shape, F32)
    act, new_master, new_moment, new_variance, scales = pl.pallas_call(
        update,
        out_shape=(
            jax.ShapeDtypeStruct((count, columns), F32),
            small, small, small,
            jax.ShapeDtypeStruct((columns // BLOCK, master.shape[0]), F32),
        ),
        in_specs=[outside] * 6,
        out_specs=(outside,) * 5,
        scratch_shapes=[
            pltpu.VMEM((count, columns), F32),
            pltpu.VMEM(piece, F32),
            pltpu.VMEM((1, columns), jnp.int32),
            pltpu.VMEM((3, *master.shape), F32),
            pltpu.VMEM((3, *master.shape), F32),
            pltpu.VMEM((columns // BLOCK, master.shape[0]), F32),
            dma((5,)), dma((2, 4)), dma((4,)),
        ],
        name="update",
    )(act, grad_t, sign_bits.reshape(1, columns), master, moment, variance)
    return act, new_master, new_moment, new_variance, scales.T


def solution(mesh):
    torus = Mesh(mesh.devices.reshape(NX, 2, 2, NZ, 2), OUTER + INNER)
    split = P(INNER, OUTER)
    return jax.shard_map(
        body, mesh=torus,
        in_specs=(split, split, P(None, OUTER), split, P(OUTER), split, split, split),
        out_specs=(split,) * 5,
        check_vma=False,
    )
```

```python
import functools

import jax
import jax.numpy as jnp
import numpy as np
from jax import lax
from jax.experimental import pallas as pl
from jax.experimental.pallas import tpu as pltpu
from jax.sharding import Mesh
from jax.sharding import PartitionSpec as P

BLOCK = 128
OUTER = ("x", "yh")
INNER = ("yl", "z", "c")
NX, NZ = 4, 8
HALF = 256
MESH = pl.DeviceIdType.MESH
F32, BF16 = jnp.float32, jnp.bfloat16


def transport(
    tokens, cotangent, cache, delta,
    act_out, grad_out,
    act, grad, tok, cot, cot_t, weight, dbuf, gbuf, grcv, zsnd, zmid, zrcv, zloc, ysnd, yrcv, yin,
    load_sem, tok_send, tok_recv, d2d_send, d2d_recv, z_send, m_recv, z_recv, y_send, y_recv,
    late_send, late_recv, dy_sem, dz_send, dz_recv, dc_send, dc_recv,
):
    x, yh, yl = lax.axis_index("x"), lax.axis_index("yh"), lax.axis_index("yl")
    z, c = lax.axis_index("z"), lax.axis_index("c")
    right, left = {"x": (x + 1) % NX}, {"x": (x + 3) % NX}
    across, beside, sibling = {"yh": 1 - yh}, {"yl": 1 - yl}, {"c": 1 - c}
    up, down = {"z": (z + 1) % NZ}, {"z": (z + 7) % NZ}

    def slot(dx, dy, half):
        row = yh if dy == 0 else 1 - yh
        return 4 * ((x + dx) % NX) + 2 * row + half

    own_a, own_b = slot(0, 0, 0), slot(0, 0, 1)
    l_a, l_b, r_a, r_b = slot(3, 0, 0), slot(3, 0, 1), slot(1, 0, 0), slot(1, 0, 1)
    ll_a, ll_b = slot(2, 0, 0), slot(2, 0, 1)
    p_a, p_b = slot(0, 1, 0), slot(0, 1, 1)
    pl_a, pl_b, pr_a, pr_b = slot(3, 1, 0), slot(3, 1, 1), slot(1, 1, 0), slot(1, 1, 1)
    pll_a, pll_b = slot(2, 1, 0), slot(2, 1, 1)

    loads = [
        pltpu.make_async_copy(
            tokens.at[:, pl.ds(BLOCK * k, BLOCK)], tok.at[2 * own_a + k], load_sem.at[k]
        )
        for k in range(4)
    ]
    load_cot = pltpu.make_async_copy(cotangent, cot, load_sem.at[4])
    load_delta = pltpu.make_async_copy(delta, dbuf.at[z, c, yl], load_sem.at[5])
    load_cache = pltpu.make_async_copy(cache, weight, load_sem.at[6])
    for copy in (load_delta, *loads, load_cot, load_cache):
        copy.start()

    barrier = pltpu.get_barrier_semaphore()
    peers = [right, left, across, beside, sibling]
    peers += [{"z": (z + step) % NZ} for step in range(1, NZ)]
    for peer in peers:
        pl.semaphore_signal(barrier, inc=1, device_id=peer, device_id_type=MESH)
    pl.semaphore_wait(barrier, len(peers))

    way = {"right": (0, right), "left": (1, left), "across": (2, across)}

    def token_copy(place, direction, part=None):
        lane, peer = way[direction]
        first = 2 * place if part is None else 2 * place + part
        piece = pl.ds(first, 2 if part is None else 1)
        return pltpu.make_async_remote_copy(
            src_ref=tok.at[piece], dst_ref=tok.at[piece],
            send_sem=tok_send.at[lane], recv_sem=tok_recv.at[first],
            device_id=peer, device_id_type=MESH,
        )

    def send(place, direction, part=None):
        token_copy(place, direction, part).start()

    def arrived(place, part=None):
        token_copy(place, "right", part).wait_recv()

    def d2d_copy(place):
        return pltpu.make_async_remote_copy(
            src_ref=gbuf.at[place, 1 - c], dst_ref=grcv.at[place],
            send_sem=d2d_send, recv_sem=d2d_recv.at[place],
            device_id=sibling, device_id_type=MESH,
        )

    def target(place):
        block = place // 2
        return block // 4, 2 * (block % 4) + place % 2

    def offset(place):
        return (z - target(place)[1] + NZ) % NZ

    def mid_copy(place):
        away, depth = offset(place), target(place)[1]
        far = jnp.where(away == 4, 1, 0)
        side = jnp.where(away == 3, 2, jnp.where(away == 5, 6, 2 + 4 * (place % 2)))
        return pltpu.make_async_remote_copy(
            src_ref=zsnd.at[place], dst_ref=zmid.at[place, far],
            send_sem=z_send.at[place], recv_sem=m_recv.at[place, far],
            device_id={"z": (depth + side) % NZ}, device_id_type=MESH,
        )

    def z_copy(place):
        rows, depth = target(place)
        away = offset(place)
        entry = jnp.where(away < 3, away - 1, away - 4)
        return pltpu.make_async_remote_copy(
            src_ref=zsnd.at[place], dst_ref=zrcv.at[rows, entry],
            send_sem=z_send.at[place], recv_sem=z_recv.at[rows, entry],
            device_id={"z": depth}, device_id_type=MESH,
        )

    def pick(places, i):
        value = places[0]
        for k in range(1, len(places)):
            value = jnp.where(i == k, places[k], value)
        return value

    late = (pr_a, pr_b, pll_a, pl_b, pll_b)

    def is_late(place):
        found = place == late[0]
        for other in late[1:]:
            found = found | (place == other)
        return found

    def late_index(place):
        index = 0
        for k in range(1, len(late)):
            index = jnp.where(place == late[k], k, index)
        return index

    def late_copy(place):
        k = late_index(place)
        return pltpu.make_async_remote_copy(
            src_ref=zsnd.at[place], dst_ref=yin.at[k],
            send_sem=late_send.at[k], recv_sem=late_recv.at[k],
            device_id=beside, device_id_type=MESH,
        )

    def dispatch(place, total):
        away = offset(place)
        zsnd[place] = total.astype(BF16)

        @pl.when((away == 1) | (away == 7))
        def _():
            z_copy(place).start()

        @pl.when((away >= 3) & (away <= 5))
        def _():
            mid_copy(place).start()

        @pl.when((away == 2) | (away == 6))
        def _():
            gbuf[place, c] = total

        @pl.when(away == 0)
        def _():
            zloc[target(place)[0]] = total

    def merge(place):
        d2d_copy(place).wait_recv()
        dispatch(place, gbuf[place, c] + grcv[place])

    def merge_late(place):
        d2d_copy(place).wait_recv()
        total = gbuf[place, c] + grcv[place]

        @pl.when(target(place)[0] != yl)
        def _():
            zsnd[place] = total.astype(BF16)
            late_copy(place).start()

        @pl.when(target(place)[0] == yl)
        def _():
            gbuf[place, c] = total

    def finish_late(*places):
        def finish(i, carry):
            place = pick(places, i)

            @pl.when(target(place)[0] == yl)
            def _():
                late_copy(place).wait_recv()
                dispatch(place, gbuf[place, c] + yin[late_index(place)].astype(F32))

            return carry

        lax.fori_loop(0, len(places), finish, 0)

    def gradients(*places, combine=merge):
        def product(i, carry):
            place = pick(places, i)
            both = jnp.concatenate([tok[2 * place], tok[2 * place + 1]], axis=1)
            terms = jnp.dot(cot_t[...], both, preferred_element_type=F32)
            gbuf[place, 0] = terms[:, :BLOCK]
            gbuf[place, 1] = terms[:, BLOCK:]
            d2d_copy(place).start()
            return carry

        def finish(i, carry):
            combine(pick(places, i))
            return carry

        lax.fori_loop(0, len(places), product, 0)
        lax.fori_loop(0, len(places), finish, 0)

    def quarters(part, *places):
        def product(i, carry):
            place = pick(places, i)
            terms = jnp.dot(cot_t[...], tok[2 * place + part], preferred_element_type=F32)
            gbuf[place, part] = terms

            @pl.when(c != part)
            def _():
                d2d_copy(place).start()

            return carry

        def finish(i, carry):
            @pl.when(c == part)
            def _():
                merge_late(pick(places, i))

            return carry

        lax.fori_loop(0, len(places), product, 0)
        lax.fori_loop(0, len(places), finish, 0)

    def relays(*places, everywhere=True):
        def relay(i, carry):
            place = pick(places, i)
            here = everywhere | (target(place)[0] == yl)
            away = jnp.where(here, offset(place), 0)

            def inflow(far):
                return pltpu.make_async_remote_copy(
                    src_ref=zmid.at[place, far], dst_ref=zmid.at[place, far],
                    send_sem=z_send.at[place], recv_sem=m_recv.at[place, far],
                    device_id=up, device_id_type=MESH,
                )

            @pl.when(away == 2 + 4 * (place % 2))
            def _():
                inflow(1).wait_recv()
                gbuf[place, c] += zmid[place, 1].astype(F32)

            @pl.when((away == 2) | (away == 6))
            def _():
                inflow(0).wait_recv()
                zsnd[place] = (gbuf[place, c] + zmid[place, 0].astype(F32)).astype(BF16)
                z_copy(place).start()

            return carry

        lax.fori_loop(0, len(places), relay, 0)

    def dz_copy(origin, peer):
        return pltpu.make_async_remote_copy(
            src_ref=dbuf.at[origin, c], dst_ref=dbuf.at[origin, c],
            send_sem=dz_send, recv_sem=dz_recv.at[origin],
            device_id=peer, device_id_type=MESH,
        )

    def dc_copy(origin):
        return pltpu.make_async_remote_copy(
            src_ref=dbuf.at[origin, c], dst_ref=dbuf.at[origin, c],
            send_sem=dc_send, recv_sem=dc_recv,
            device_id=sibling, device_id_type=MESH,
        )

    dy_copy = pltpu.make_async_remote_copy(
        src_ref=dbuf.at[z, c, yl], dst_ref=dbuf.at[z, c, yl],
        send_sem=dy_sem.at[0], recv_sem=dy_sem.at[1],
        device_id=beside, device_id_type=MESH,
    )
    dy_in = pltpu.make_async_remote_copy(
        src_ref=dbuf.at[z, c, 1 - yl], dst_ref=dbuf.at[z, c, 1 - yl],
        send_sem=dy_sem.at[0], recv_sem=dy_sem.at[1],
        device_id=beside, device_id_type=MESH,
    )

    def delta_step(step):
        below, above = (z + NZ - step) % NZ, (z + step) % NZ
        if step == 0:
            dy_in.wait_recv()
        else:
            dz_copy(below, up).wait_recv()
        if step < 4:
            dz_copy(below, up).start()
        dc_copy(below).start()
        if 0 < step < 4:
            dz_copy(above, down).wait_recv()
        if step < 3:
            dz_copy(above, down).start()
        if 0 < step < 4:
            dc_copy(above).start()

    def rebuild(j, carry):
        rows = pl.ds(pl.multiple_of(j * BLOCK, BLOCK), BLOCK)
        change = dbuf[(j % 16) // 2, j % 2, j // 16]
        weight[rows, :] = (weight[rows, :].astype(F32) + change.astype(F32)).astype(BF16)
        return carry

    def project(*firsts):
        def add(i, carry):
            first = pick(firsts, i)
            rows = pl.ds(pl.multiple_of(first * HALF, HALF), 2 * HALF)
            block = jnp.concatenate([tok[2 * first + k] for k in range(4)], axis=1)
            act[...] += jnp.dot(block, weight[rows, :], preferred_element_type=F32)
            return carry

        lax.fori_loop(0, len(firsts), add, 0)

    load_delta.wait()
    dy_copy.start()
    loads[0].wait()
    loads[1].wait()
    send(own_a, "right")
    send(own_a, "across")
    loads[2].wait()
    loads[3].wait()
    send(own_b, "left")
    send(own_b, "right")
    send(own_a, "left")
    load_cot.wait()
    cot_t[...] = cot[...].T
    gradients(own_a, own_b)
    delta_step(0)
    act[...] = jnp.zeros_like(act)

    arrived(l_a)
    send(l_a, "right")
    send(l_a, "across")
    send(own_b, "across")
    arrived(r_b)
    send(r_b, "left")
    send(r_b, "across", 0)
    send(r_b, "across", 1)
    arrived(p_a)
    send(p_a, "left")
    delta_step(1)
    gradients(l_a, r_b, p_a)
    relays(own_a, own_b)

    arrived(l_b)
    arrived(r_a)
    arrived(pl_a)
    send(pl_a, "right")
    delta_step(2)
    gradients(l_b, r_a, pl_a)
    relays(l_a, r_b, p_a)

    arrived(ll_a)
    arrived(ll_b)
    arrived(p_b)
    send(p_b, "right", 0)
    send(p_b, "right", 1)
    delta_step(3)
    gradients(ll_a, ll_b, p_b)
    relays(l_b, r_a, pl_a)

    arrived(pr_b, 0)
    send(pr_b, "left", 0)
    arrived(pr_b, 1)
    send(pr_b, "left", 1)
    relays(ll_a, ll_b, p_b)
    delta_step(4)
    arrived(pr_a)
    arrived(pll_a)
    gradients(pr_a, pr_b, pll_a, combine=merge_late)

    arrived(pl_b, 0)
    arrived(pll_b, 0)
    quarters(0, pl_b, pll_b)
    load_cache.wait()
    pltpu.make_async_remote_copy(
        src_ref=dbuf.at[:, 1 - c], dst_ref=dbuf.at[:, 1 - c],
        send_sem=dc_send, recv_sem=dc_recv,
        device_id=sibling, device_id_type=MESH,
    ).wait_recv()
    lax.fori_loop(0, 32, rebuild, 0)
    arrived(pl_b, 1)
    arrived(pll_b, 1)
    quarters(1, pl_b, pll_b)
    finish_late(pr_a, pr_b, pll_a)
    project(own_a, l_a)
    finish_late(pl_b, pll_b)

    def collected(rows):
        total = zloc[rows]
        for entry in range(4):
            pltpu.make_async_remote_copy(
                src_ref=zrcv.at[rows, entry], dst_ref=zrcv.at[rows, entry],
                send_sem=z_send.at[0], recv_sem=z_recv.at[rows, entry],
                device_id=up, device_id_type=MESH,
            ).wait_recv()
            total = total + zrcv[rows, entry].astype(F32)
        return total

    mine, other = [8 * row + z for row in (yl, 1 - yl)]
    y_copy = pltpu.make_async_remote_copy(
        src_ref=ysnd, dst_ref=yrcv, send_sem=y_send, recv_sem=y_recv,
        device_id=beside, device_id_type=MESH,
    )
    early_out, early_in = jnp.logical_not(is_late(other)), jnp.logical_not(is_late(mine))

    @pl.when(early_out)
    def _():
        ysnd[...] = collected(1 - yl).astype(BF16)
        y_copy.start()

    project(r_a, p_a)
    relays(pr_a, pr_b, pll_a, everywhere=False)
    relays(pl_b, pll_b, everywhere=False)
    project(ll_a, pr_a, pl_a, pll_a)
    store_act = pltpu.make_async_copy(act, act_out, load_sem.at[7])
    store_act.start()

    grad[...] = collected(yl)

    @pl.when(early_in)
    def _():
        y_copy.wait_recv()
        grad[...] += yrcv[...].astype(F32)

    store_grad = pltpu.make_async_copy(grad, grad_out, load_sem.at[8])
    store_grad.start()

    @pl.when(early_out)
    def _():
        y_copy.wait_send()

    dy_copy.wait_send()
    def sent(block, sem):
        pltpu.make_async_remote_copy(
            src_ref=block, dst_ref=block, send_sem=sem, recv_sem=y_recv,
            device_id=beside, device_id_type=MESH,
        ).wait_send()

    sent(tok.at[pl.ds(0, 10)], tok_send.at[0])
    sent(tok.at[pl.ds(0, 10)], tok_send.at[1])
    sent(tok.at[pl.ds(0, 8)], tok_send.at[2])
    sent(dbuf.at[pl.ds(0, 7), c], dz_send)
    sent(dbuf.at[:, c], dc_send)
    sent(grcv, d2d_send)

    def drain(place, carry):
        aside = is_late(place) & (target(place)[0] != yl)

        @pl.when(aside)
        def _():
            late_copy(place).wait_send()

        @pl.when(jnp.logical_not(aside) & (offset(place) != 0))
        def _():
            sent(zsnd.at[place], z_send.at[place])

        return carry

    lax.fori_loop(0, 16, drain, 0)
    store_act.wait()
    store_grad.wait()


def hadamard(length):
    first = lax.broadcasted_iota(jnp.int32, (length, length), 0)
    second = lax.broadcasted_iota(jnp.int32, (length, length), 1)
    common = jnp.bitwise_and(first, second)
    parity = jnp.zeros((length, length), jnp.int32)
    for place in range(length.bit_length() - 1):
        parity = parity + jnp.bitwise_and(jnp.right_shift(common, place), 1)
    signs = (1 - 2 * jnp.bitwise_and(parity, 1)).astype(F32)
    return signs / np.sqrt(np.float32(length))


def update(
    act_in, grad_t, sign_bits, master, moment, variance,
    act, new_master, new_moment, new_variance, scales,
    held, grad, bits, old, out, peaks, sem_in, sem_held, sem_out,
):
    pieces = 4
    rows = held.shape[0] // pieces
    spans = [pl.ds(k * rows, rows) for k in range(pieces)]
    fetches = [
        pltpu.make_async_copy(source, target, sem_in.at[k])
        for k, (source, target) in enumerate((
            (grad_t, grad), (sign_bits, bits), (master, old.at[0]), (moment, old.at[1]), (variance, old.at[2])
        ))
    ]
    moves = [
        (
            pltpu.make_async_copy(act_in.at[span], held.at[span], sem_held.at[0, k]),
            pltpu.make_async_copy(held.at[span], act.at[span], sem_held.at[1, k]),
        )
        for k, span in enumerate(spans)
    ]
    for copy in fetches:
        copy.start()
    for fetch, _ in moves:
        fetch.start()
    table = hadamard(BLOCK)
    for copy in fetches:
        copy.wait()
    for fetch, store in moves:
        fetch.wait()
        store.start()
    for k in range(old.shape[2] // BLOCK):
        span = pl.ds(k * BLOCK, BLOCK)
        signs = (1 - 2 * bits[:, span]).astype(F32)
        gradient = grad[span, :].T
        smoothed = jnp.dot(
            gradient * signs, table, precision=lax.Precision.HIGHEST, preferred_element_type=F32
        )
        peaks[pl.ds(k, 1), :] = jnp.max(jnp.abs(smoothed.T), axis=0, keepdims=True)
        restored = signs * jnp.dot(
            smoothed, table, precision=lax.Precision.HIGHEST, preferred_element_type=F32
        )
        first = 0.9 * old[1, :, span] + 0.1 * restored
        second = 0.95 * old[2, :, span] + 0.05 * restored * restored
        corrected = first / (1.0 - 0.9**10)
        spread = jnp.sqrt(second / (1.0 - 0.95**10)) + 1e-08
        weight = old[0, :, span]
        out[0, :, span] = weight - 0.01 * (corrected / spread + 0.1 * weight)
        out[1, :, span] = first
        out[2, :, span] = second
    stores = [
        pltpu.make_async_copy(out.at[k], target, sem_out.at[k])
        for k, target in enumerate((new_master, new_moment, new_variance))
    ]
    stores.append(pltpu.make_async_copy(peaks, scales, sem_out.at[3]))
    for copy in stores:
        copy.start()
    for _, store in moves:
        store.wait()
    for copy in stores:
        copy.wait()


def body(tokens, cotangent, weight_cache, weight_delta, sign_bits, master, moment, variance):
    count, width = tokens.shape
    columns = cotangent.shape[1]
    inside = pl.BlockSpec(memory_space=pltpu.VMEM)
    outside = pl.BlockSpec(memory_space=pltpu.HBM)
    dma = pltpu.SemaphoreType.DMA
    piece = (columns, BLOCK)
    act, grad_t = pl.pallas_call(
        transport,
        out_shape=(
            jax.ShapeDtypeStruct((count, columns), F32),
            jax.ShapeDtypeStruct(piece, F32),
        ),
        in_specs=[outside] * 4,
        out_specs=(outside, outside),
        scratch_shapes=[
            pltpu.VMEM((count, columns), F32),
            pltpu.VMEM(piece, F32),
            pltpu.VMEM((32, count, BLOCK), BF16),
            pltpu.VMEM((count, columns), BF16),
            pltpu.VMEM((columns, count), BF16),
            pltpu.VMEM(weight_cache.shape, BF16),
            pltpu.VMEM((NZ, 2, 2, BLOCK, columns), BF16),
            pltpu.VMEM((16, 2, *piece), F32),
            pltpu.VMEM((16, *piece), F32),
            pltpu.VMEM((16, *piece), BF16),
            pltpu.VMEM((16, 2, *piece), BF16),
            pltpu.VMEM((2, 4, *piece), BF16),
            pltpu.VMEM((2, *piece), F32),
            pltpu.VMEM(piece, BF16),
            pltpu.VMEM(piece, BF16),
            pltpu.VMEM((5, *piece), BF16),
            dma((9,)), dma((3,)), dma((32,)), dma, dma((16,)), dma((16,)),
            dma((16, 2)), dma((2, 4)), dma, dma, dma((5,)), dma((5,)), dma((2,)), dma, dma((NZ,)), dma, dma,
        ],
        compiler_params=pltpu.CompilerParams(
            collective_id=0, has_side_effects=True, vmem_limit_bytes=58 * 2**20
        ),
        name="transport",
    )(tokens, cotangent, weight_cache, weight_delta)
    small = jax.ShapeDtypeStruct(master.shape, F32)
    act, new_master, new_moment, new_variance, scales = pl.pallas_call(
        update,
        out_shape=(
            jax.ShapeDtypeStruct((count, columns), F32),
            small, small, small,
            jax.ShapeDtypeStruct((columns // BLOCK, master.shape[0]), F32),
        ),
        in_specs=[outside] * 6,
        out_specs=(outside,) * 5,
        scratch_shapes=[
            pltpu.VMEM((count, columns), F32),
            pltpu.VMEM(piece, F32),
            pltpu.VMEM((1, columns), jnp.int32),
            pltpu.VMEM((3, *master.shape), F32),
            pltpu.VMEM((3, *master.shape), F32),
            pltpu.VMEM((columns // BLOCK, master.shape[0]), F32),
            dma((5,)), dma((2, 4)), dma((4,)),
        ],
        name="update",
    )(act, grad_t, sign_bits.reshape(1, columns), master, moment, variance)
    return act, new_master, new_moment, new_variance, scales.T


def solution(mesh):
    torus = Mesh(mesh.devices.reshape(NX, 2, 2, NZ, 2), OUTER + INNER)
    split = P(INNER, OUTER)
    return jax.shard_map(
        body, mesh=torus,
        in_specs=(split, split, P(None, OUTER), split, P(OUTER), split, split, split),
        out_specs=(split,) * 5,
        check_vma=False,
    )
```

```python
import functools

import jax
import jax.numpy as jnp
import numpy as np
from jax import lax
from jax.experimental import pallas as pl
from jax.experimental.pallas import tpu as pltpu
from jax.sharding import Mesh
from jax.sharding import PartitionSpec as P

BLOCK = 128
OUTER = ("x", "yh")
INNER = ("yl", "z", "c")
NX, NZ = 4, 8
HALF = 256
MESH = pl.DeviceIdType.MESH
F32, BF16 = jnp.float32, jnp.bfloat16


def transport(
    tokens, cotangent, cache, delta,
    act_out, grad_out,
    act, grad, tok, cot, cot_t, weight, dbuf, gbuf, grcv, zsnd, zmid, zrcv, zloc, ysnd, yrcv, yin,
    load_sem, tok_send, tok_recv, d2d_send, d2d_recv, z_send, m_recv, z_recv, y_send, y_recv,
    late_send, late_recv, dy_sem, dz_send, dz_recv, dc_send, dc_recv,
):
    x, yh, yl = lax.axis_index("x"), lax.axis_index("yh"), lax.axis_index("yl")
    z, c = lax.axis_index("z"), lax.axis_index("c")
    right, left = {"x": (x + 1) % NX}, {"x": (x + 3) % NX}
    across, beside, sibling = {"yh": 1 - yh}, {"yl": 1 - yl}, {"c": 1 - c}
    up, down = {"z": (z + 1) % NZ}, {"z": (z + 7) % NZ}

    def slot(dx, dy, half):
        row = yh if dy == 0 else 1 - yh
        return 4 * ((x + dx) % NX) + 2 * row + half

    own_a, own_b = slot(0, 0, 0), slot(0, 0, 1)
    l_a, l_b, r_a, r_b = slot(3, 0, 0), slot(3, 0, 1), slot(1, 0, 0), slot(1, 0, 1)
    ll_a, ll_b = slot(2, 0, 0), slot(2, 0, 1)
    p_a, p_b = slot(0, 1, 0), slot(0, 1, 1)
    pl_a, pl_b, pr_a, pr_b = slot(3, 1, 0), slot(3, 1, 1), slot(1, 1, 0), slot(1, 1, 1)
    pll_a, pll_b = slot(2, 1, 0), slot(2, 1, 1)

    loads = [
        pltpu.make_async_copy(
            tokens.at[:, pl.ds(BLOCK * k, BLOCK)], tok.at[2 * own_a + k], load_sem.at[k]
        )
        for k in range(4)
    ]
    load_cot = pltpu.make_async_copy(cotangent, cot, load_sem.at[4])
    load_delta = pltpu.make_async_copy(delta, dbuf.at[z, c, yl], load_sem.at[5])
    load_cache = pltpu.make_async_copy(cache, weight, load_sem.at[6])
    for copy in (load_delta, *loads, load_cot, load_cache):
        copy.start()

    barrier = pltpu.get_barrier_semaphore()
    peers = [right, left, across, beside, sibling]
    peers += [{"z": (z + step) % NZ} for step in range(1, NZ)]
    for peer in peers:
        pl.semaphore_signal(barrier, inc=1, device_id=peer, device_id_type=MESH)
    pl.semaphore_wait(barrier, len(peers))

    way = {"right": (0, right), "left": (1, left), "across": (2, across)}

    def token_copy(place, direction, part=None):
        lane, peer = way[direction]
        first = 2 * place if part is None else 2 * place + part
        piece = pl.ds(first, 2 if part is None else 1)
        return pltpu.make_async_remote_copy(
            src_ref=tok.at[piece], dst_ref=tok.at[piece],
            send_sem=tok_send.at[lane], recv_sem=tok_recv.at[first],
            device_id=peer, device_id_type=MESH,
        )

    def send(place, direction, part=None):
        token_copy(place, direction, part).start()

    def arrived(place, part=None):
        token_copy(place, "right", part).wait_recv()

    def d2d_copy(place):
        return pltpu.make_async_remote_copy(
            src_ref=gbuf.at[place, 1 - c], dst_ref=grcv.at[place],
            send_sem=d2d_send, recv_sem=d2d_recv.at[place],
            device_id=sibling, device_id_type=MESH,
        )

    def target(place):
        block = place // 2
        return block // 4, 2 * (block % 4) + place % 2

    def offset(place):
        return (z - target(place)[1] + NZ) % NZ

    def mid_copy(place):
        away = offset(place)
        rows, depth = target(place)
        far = jnp.where(away == 4, 1, 0)
        side = jnp.where(away == 3, 2, jnp.where(away == 5, 6, 2 + 4 * (place % 2)))
        return pltpu.make_async_remote_copy(
            src_ref=zsnd.at[place], dst_ref=zmid.at[rows, side // 4, far],
            send_sem=z_send.at[place], recv_sem=m_recv.at[rows, side // 4, far],
            device_id={"z": (depth + side) % NZ}, device_id_type=MESH,
        )

    def z_copy(place):
        rows, depth = target(place)
        away = offset(place)
        entry = jnp.where(away < 3, away - 1, away - 4)
        return pltpu.make_async_remote_copy(
            src_ref=zsnd.at[place], dst_ref=zrcv.at[rows, entry],
            send_sem=z_send.at[place], recv_sem=z_recv.at[rows, entry],
            device_id={"z": depth}, device_id_type=MESH,
        )

    def pick(places, i):
        value = places[0]
        for k in range(1, len(places)):
            value = jnp.where(i == k, places[k], value)
        return value

    late = (pr_a, pr_b, pll_a, pl_b, pll_b)

    def is_late(place):
        found = place == late[0]
        for other in late[1:]:
            found = found | (place == other)
        return found

    def late_index(place):
        index = 0
        for k in range(1, len(late)):
            index = jnp.where(place == late[k], k, index)
        return index

    def late_copy(place):
        k = late_index(place)
        return pltpu.make_async_remote_copy(
            src_ref=zsnd.at[place], dst_ref=yin.at[k],
            send_sem=late_send.at[k], recv_sem=late_recv.at[k],
            device_id=beside, device_id_type=MESH,
        )

    def dispatch(place, total):
        away = offset(place)
        zsnd[place] = total.astype(BF16)

        @pl.when((away == 1) | (away == 7))
        def _():
            z_copy(place).start()

        @pl.when((away >= 3) & (away <= 5))
        def _():
            mid_copy(place).start()

        @pl.when((away == 2) | (away == 6))
        def _():
            gbuf[place, c] = total

        @pl.when(away == 0)
        def _():
            zloc[target(place)[0]] = total

    def merge(place):
        d2d_copy(place).wait_recv()
        dispatch(place, gbuf[place, c] + grcv[place])

    def merge_late(place):
        d2d_copy(place).wait_recv()
        total = gbuf[place, c] + grcv[place]

        @pl.when(target(place)[0] != yl)
        def _():
            zsnd[place] = total.astype(BF16)
            late_copy(place).start()

        @pl.when(target(place)[0] == yl)
        def _():
            gbuf[place, c] = total

    def finish_late(*places):
        def finish(i, carry):
            place = pick(places, i)

            @pl.when(target(place)[0] == yl)
            def _():
                late_copy(place).wait_recv()
                dispatch(place, gbuf[place, c] + yin[late_index(place)].astype(F32))

            return carry

        lax.fori_loop(0, len(places), finish, 0)

    def gradients(*places, combine=merge):
        def product(i, carry):
            place = pick(places, i)
            both = jnp.concatenate([tok[2 * place], tok[2 * place + 1]], axis=1)
            terms = jnp.dot(cot_t[...], both, preferred_element_type=F32)
            gbuf[place, 0] = terms[:, :BLOCK]
            gbuf[place, 1] = terms[:, BLOCK:]
            d2d_copy(place).start()
            return carry

        def finish(i, carry):
            combine(pick(places, i))
            return carry

        lax.fori_loop(0, len(places), product, 0)
        lax.fori_loop(0, len(places), finish, 0)

    def quarters(part, *places):
        def product(i, carry):
            place = pick(places, i)
            terms = jnp.dot(cot_t[...], tok[2 * place + part], preferred_element_type=F32)
            gbuf[place, part] = terms

            @pl.when(c != part)
            def _():
                d2d_copy(place).start()

            return carry

        def finish(i, carry):
            @pl.when(c == part)
            def _():
                merge_late(pick(places, i))

            return carry

        lax.fori_loop(0, len(places), product, 0)
        lax.fori_loop(0, len(places), finish, 0)

    def relays(*places, everywhere=True):
        def relay(i, carry):
            place = pick(places, i)
            here = everywhere | (target(place)[0] == yl)
            away = jnp.where(here, offset(place), 0)

            rows, side = target(place)[0], away // 4

            def inflow(far):
                return pltpu.make_async_remote_copy(
                    src_ref=zmid.at[rows, side, far], dst_ref=zmid.at[rows, side, far],
                    send_sem=z_send.at[place], recv_sem=m_recv.at[rows, side, far],
                    device_id=up, device_id_type=MESH,
                )

            @pl.when(away == 2 + 4 * (place % 2))
            def _():
                inflow(1).wait_recv()
                gbuf[place, c] += zmid[rows, side, 1].astype(F32)

            @pl.when((away == 2) | (away == 6))
            def _():
                inflow(0).wait_recv()
                zsnd[place] = (gbuf[place, c] + zmid[rows, side, 0].astype(F32)).astype(BF16)
                z_copy(place).start()

            return carry

        lax.fori_loop(0, len(places), relay, 0)

    def dz_copy(origin, peer):
        return pltpu.make_async_remote_copy(
            src_ref=dbuf.at[origin, c], dst_ref=dbuf.at[origin, c],
            send_sem=dz_send, recv_sem=dz_recv.at[origin],
            device_id=peer, device_id_type=MESH,
        )

    def dc_copy(origin):
        return pltpu.make_async_remote_copy(
            src_ref=dbuf.at[origin, c], dst_ref=dbuf.at[origin, c],
            send_sem=dc_send, recv_sem=dc_recv,
            device_id=sibling, device_id_type=MESH,
        )

    dy_copy = pltpu.make_async_remote_copy(
        src_ref=dbuf.at[z, c, yl], dst_ref=dbuf.at[z, c, yl],
        send_sem=dy_sem.at[0], recv_sem=dy_sem.at[1],
        device_id=beside, device_id_type=MESH,
    )
    dy_in = pltpu.make_async_remote_copy(
        src_ref=dbuf.at[z, c, 1 - yl], dst_ref=dbuf.at[z, c, 1 - yl],
        send_sem=dy_sem.at[0], recv_sem=dy_sem.at[1],
        device_id=beside, device_id_type=MESH,
    )

    def delta_step(step):
        below, above = (z + NZ - step) % NZ, (z + step) % NZ
        if step == 0:
            dy_in.wait_recv()
        else:
            dz_copy(below, up).wait_recv()
        if step < 4:
            dz_copy(below, up).start()
        dc_copy(below).start()
        if 0 < step < 4:
            dz_copy(above, down).wait_recv()
        if step < 3:
            dz_copy(above, down).start()
        if 0 < step < 4:
            dc_copy(above).start()

    def rebuild(j, carry):
        rows = pl.ds(pl.multiple_of(j * BLOCK, BLOCK), BLOCK)
        change = dbuf[(j % 16) // 2, j % 2, j // 16]
        weight[rows, :] = (weight[rows, :].astype(F32) + change.astype(F32)).astype(BF16)
        return carry

    def project(*firsts):
        def add(i, carry):
            first = pick(firsts, i)
            rows = pl.ds(pl.multiple_of(first * HALF, HALF), 2 * HALF)
            block = jnp.concatenate([tok[2 * first + k] for k in range(4)], axis=1)
            act[...] += jnp.dot(block, weight[rows, :], preferred_element_type=F32)
            return carry

        lax.fori_loop(0, len(firsts), add, 0)

    load_delta.wait()
    dy_copy.start()
    loads[0].wait()
    loads[1].wait()
    send(own_a, "right")
    send(own_a, "across")
    loads[2].wait()
    loads[3].wait()
    send(own_b, "left")
    send(own_b, "right")
    send(own_a, "left")
    load_cot.wait()
    cot_t[...] = cot[...].T
    gradients(own_a, own_b)
    delta_step(0)
    act[...] = jnp.zeros_like(act)

    arrived(l_a)
    send(l_a, "right")
    send(l_a, "across")
    send(own_b, "across")
    arrived(r_b)
    send(r_b, "left")
    send(r_b, "across", 0)
    send(r_b, "across", 1)
    arrived(p_a)
    send(p_a, "left")
    delta_step(1)
    gradients(l_a, r_b, p_a)
    relays(own_a, own_b)

    arrived(l_b)
    arrived(r_a)
    arrived(pl_a)
    send(pl_a, "right")
    delta_step(2)
    gradients(l_b, r_a, pl_a)
    relays(l_a, r_b, p_a)

    arrived(ll_a)
    arrived(ll_b)
    arrived(p_b)
    send(p_b, "right", 0)
    send(p_b, "right", 1)
    delta_step(3)
    gradients(ll_a, ll_b, p_b)
    relays(l_b, r_a, pl_a)

    arrived(pr_b, 0)
    send(pr_b, "left", 0)
    arrived(pr_a)
    arrived(pll_a)
    gradients(pr_a, pll_a, combine=merge_late)
    arrived(pr_b, 1)
    send(pr_b, "left", 1)
    gradients(pr_b, combine=merge_late)
    relays(ll_a, ll_b, p_b)
    delta_step(4)

    arrived(pl_b, 0)
    arrived(pll_b, 0)
    quarters(0, pl_b, pll_b)
    load_cache.wait()
    pltpu.make_async_remote_copy(
        src_ref=dbuf.at[:, 1 - c], dst_ref=dbuf.at[:, 1 - c],
        send_sem=dc_send, recv_sem=dc_recv,
        device_id=sibling, device_id_type=MESH,
    ).wait_recv()
    finish_late(pr_a, pll_a)
    lax.fori_loop(0, 32, rebuild, 0)
    arrived(pl_b, 1)
    arrived(pll_b, 1)
    quarters(1, pl_b, pll_b)
    finish_late(pr_b)
    project(own_a, l_a)
    finish_late(pl_b, pll_b)

    def collected(rows):
        total = zloc[rows]
        for entry in range(4):
            pltpu.make_async_remote_copy(
                src_ref=zrcv.at[rows, entry], dst_ref=zrcv.at[rows, entry],
                send_sem=z_send.at[0], recv_sem=z_recv.at[rows, entry],
                device_id=up, device_id_type=MESH,
            ).wait_recv()
            total = total + zrcv[rows, entry].astype(F32)
        return total

    mine, other = [8 * row + z for row in (yl, 1 - yl)]
    y_copy = pltpu.make_async_remote_copy(
        src_ref=ysnd, dst_ref=yrcv, send_sem=y_send, recv_sem=y_recv,
        device_id=beside, device_id_type=MESH,
    )
    early_out, early_in = jnp.logical_not(is_late(other)), jnp.logical_not(is_late(mine))

    @pl.when(early_out)
    def _():
        ysnd[...] = collected(1 - yl).astype(BF16)
        y_copy.start()

    project(r_a, p_a)
    relays(pr_a, pr_b, pll_a, everywhere=False)
    relays(pl_b, pll_b, everywhere=False)
    project(ll_a, pr_a, pl_a, pll_a)
    store_act = pltpu.make_async_copy(act, act_out, load_sem.at[7])
    store_act.start()

    grad[...] = collected(yl)

    @pl.when(early_in)
    def _():
        y_copy.wait_recv()
        grad[...] += yrcv[...].astype(F32)

    store_grad = pltpu.make_async_copy(grad, grad_out, load_sem.at[8])
    store_grad.start()

    @pl.when(early_out)
    def _():
        y_copy.wait_send()

    dy_copy.wait_send()
    def sent(block, sem):
        pltpu.make_async_remote_copy(
            src_ref=block, dst_ref=block, send_sem=sem, recv_sem=y_recv,
            device_id=beside, device_id_type=MESH,
        ).wait_send()

    sent(tok.at[pl.ds(0, 10)], tok_send.at[0])
    sent(tok.at[pl.ds(0, 10)], tok_send.at[1])
    sent(tok.at[pl.ds(0, 8)], tok_send.at[2])
    sent(dbuf.at[pl.ds(0, 7), c], dz_send)
    sent(dbuf.at[:, c], dc_send)
    sent(grcv, d2d_send)

    def drain(place, carry):
        aside = is_late(place) & (target(place)[0] != yl)

        @pl.when(aside)
        def _():
            late_copy(place).wait_send()

        @pl.when(jnp.logical_not(aside) & (offset(place) != 0))
        def _():
            sent(zsnd.at[place], z_send.at[place])

        return carry

    lax.fori_loop(0, 16, drain, 0)
    store_act.wait()
    store_grad.wait()


def hadamard(length):
    first = lax.broadcasted_iota(jnp.int32, (length, length), 0)
    second = lax.broadcasted_iota(jnp.int32, (length, length), 1)
    common = jnp.bitwise_and(first, second)
    parity = jnp.zeros((length, length), jnp.int32)
    for place in range(length.bit_length() - 1):
        parity = parity + jnp.bitwise_and(jnp.right_shift(common, place), 1)
    signs = (1 - 2 * jnp.bitwise_and(parity, 1)).astype(F32)
    return signs / np.sqrt(np.float32(length))


def update(
    act_in, grad_t, sign_bits, master, moment, variance,
    act, new_master, new_moment, new_variance, scales,
    held, grad, bits, old, out, peaks, sem_in, sem_held, sem_out,
):
    pieces = 4
    rows = held.shape[0] // pieces
    spans = [pl.ds(k * rows, rows) for k in range(pieces)]
    fetches = [
        pltpu.make_async_copy(source, target, sem_in.at[k])
        for k, (source, target) in enumerate((
            (grad_t, grad), (sign_bits, bits), (master, old.at[0]), (moment, old.at[1]), (variance, old.at[2])
        ))
    ]
    moves = [
        (
            pltpu.make_async_copy(act_in.at[span], held.at[span], sem_held.at[0, k]),
            pltpu.make_async_copy(held.at[span], act.at[span], sem_held.at[1, k]),
        )
        for k, span in enumerate(spans)
    ]
    for copy in fetches:
        copy.start()
    for fetch, _ in moves:
        fetch.start()
    table = hadamard(BLOCK)
    for copy in fetches:
        copy.wait()
    for fetch, store in moves:
        fetch.wait()
        store.start()
    for k in range(old.shape[2] // BLOCK):
        span = pl.ds(k * BLOCK, BLOCK)
        signs = (1 - 2 * bits[:, span]).astype(F32)
        gradient = grad[span, :].T
        smoothed = jnp.dot(
            gradient * signs, table, precision=lax.Precision.HIGHEST, preferred_element_type=F32
        )
        peaks[pl.ds(k, 1), :] = jnp.max(jnp.abs(smoothed.T), axis=0, keepdims=True)
        restored = signs * jnp.dot(
            smoothed, table, precision=lax.Precision.HIGHEST, preferred_element_type=F32
        )
        first = 0.9 * old[1, :, span] + 0.1 * restored
        second = 0.95 * old[2, :, span] + 0.05 * restored * restored
        corrected = first / (1.0 - 0.9**10)
        spread = jnp.sqrt(second / (1.0 - 0.95**10)) + 1e-08
        weight = old[0, :, span]
        out[0, :, span] = weight - 0.01 * (corrected / spread + 0.1 * weight)
        out[1, :, span] = first
        out[2, :, span] = second
    stores = [
        pltpu.make_async_copy(out.at[k], target, sem_out.at[k])
        for k, target in enumerate((new_master, new_moment, new_variance))
    ]
    stores.append(pltpu.make_async_copy(peaks, scales, sem_out.at[3]))
    for copy in stores:
        copy.start()
    for _, store in moves:
        store.wait()
    for copy in stores:
        copy.wait()


def body(tokens, cotangent, weight_cache, weight_delta, sign_bits, master, moment, variance):
    count, width = tokens.shape
    columns = cotangent.shape[1]
    inside = pl.BlockSpec(memory_space=pltpu.VMEM)
    outside = pl.BlockSpec(memory_space=pltpu.HBM)
    dma = pltpu.SemaphoreType.DMA
    piece = (columns, BLOCK)
    act, grad_t = pl.pallas_call(
        transport,
        out_shape=(
            jax.ShapeDtypeStruct((count, columns), F32),
            jax.ShapeDtypeStruct(piece, F32),
        ),
        in_specs=[outside] * 4,
        out_specs=(outside, outside),
        scratch_shapes=[
            pltpu.VMEM((count, columns), F32),
            pltpu.VMEM(piece, F32),
            pltpu.VMEM((32, count, BLOCK), BF16),
            pltpu.VMEM((count, columns), BF16),
            pltpu.VMEM((columns, count), BF16),
            pltpu.VMEM(weight_cache.shape, BF16),
            pltpu.VMEM((NZ, 2, 2, BLOCK, columns), BF16),
            pltpu.VMEM((16, 2, *piece), F32),
            pltpu.VMEM((16, *piece), F32),
            pltpu.VMEM((16, *piece), BF16),
            pltpu.VMEM((2, 2, 2, *piece), BF16),
            pltpu.VMEM((2, 4, *piece), BF16),
            pltpu.VMEM((2, *piece), F32),
            pltpu.VMEM(piece, BF16),
            pltpu.VMEM(piece, BF16),
            pltpu.VMEM((5, *piece), BF16),
            dma((9,)), dma((3,)), dma((32,)), dma, dma((16,)), dma((16,)),
            dma((2, 2, 2)), dma((2, 4)), dma, dma, dma((5,)), dma((5,)), dma((2,)), dma, dma((NZ,)), dma, dma,
        ],
        compiler_params=pltpu.CompilerParams(
            collective_id=0, has_side_effects=True, vmem_limit_bytes=58 * 2**20
        ),
        name="transport",
    )(tokens, cotangent, weight_cache, weight_delta)
    small = jax.ShapeDtypeStruct(master.shape, F32)
    act, new_master, new_moment, new_variance, scales = pl.pallas_call(
        update,
        out_shape=(
            jax.ShapeDtypeStruct((count, columns), F32),
            small, small, small,
            jax.ShapeDtypeStruct((columns // BLOCK, master.shape[0]), F32),
        ),
        in_specs=[outside] * 6,
        out_specs=(outside,) * 5,
        scratch_shapes=[
            pltpu.VMEM((count, columns), F32),
            pltpu.VMEM(piece, F32),
            pltpu.VMEM((1, columns), jnp.int32),
            pltpu.VMEM((3, *master.shape), F32),
            pltpu.VMEM((3, *master.shape), F32),
            pltpu.VMEM((columns // BLOCK, master.shape[0]), F32),
            dma((5,)), dma((2, 4)), dma((4,)),
        ],
        name="update",
    )(act, grad_t, sign_bits.reshape(1, columns), master, moment, variance)
    return act, new_master, new_moment, new_variance, scales.T


def solution(mesh):
    torus = Mesh(mesh.devices.reshape(NX, 2, 2, NZ, 2), OUTER + INNER)
    split = P(INNER, OUTER)
    return jax.shard_map(
        body, mesh=torus,
        in_specs=(split, split, P(None, OUTER), split, P(OUTER), split, split, split),
        out_specs=(split,) * 5,
        check_vma=False,
    )
```

```python
import functools

import jax
import jax.numpy as jnp
import numpy as np
from jax import lax
from jax.experimental import pallas as pl
from jax.experimental.pallas import tpu as pltpu
from jax.sharding import Mesh
from jax.sharding import PartitionSpec as P

BLOCK = 128
OUTER = ("x", "yh")
INNER = ("yl", "z", "c")
NX, NZ = 4, 8
HALF = 256
MESH = pl.DeviceIdType.MESH
F32, BF16 = jnp.float32, jnp.bfloat16


def transport(
    tokens, cotangent, cache, delta,
    act, grad,
    tok, cot, cot_t, weight, dbuf, gbuf, grcv, zsnd, zmid, zrcv, zloc, ysnd, yrcv, yin,
    load_sem, tok_send, tok_recv, d2d_send, d2d_recv, z_send, m_recv, z_recv, y_send, y_recv,
    late_send, late_recv, dy_sem, dz_send, dz_recv, dc_send, dc_recv,
):
    x, yh, yl = lax.axis_index("x"), lax.axis_index("yh"), lax.axis_index("yl")
    z, c = lax.axis_index("z"), lax.axis_index("c")
    right, left = {"x": (x + 1) % NX}, {"x": (x + 3) % NX}
    across, beside, sibling = {"yh": 1 - yh}, {"yl": 1 - yl}, {"c": 1 - c}
    up, down = {"z": (z + 1) % NZ}, {"z": (z + 7) % NZ}

    def slot(dx, dy, half):
        row = yh if dy == 0 else 1 - yh
        return 4 * ((x + dx) % NX) + 2 * row + half

    own_a, own_b = slot(0, 0, 0), slot(0, 0, 1)
    l_a, l_b, r_a, r_b = slot(3, 0, 0), slot(3, 0, 1), slot(1, 0, 0), slot(1, 0, 1)
    ll_a, ll_b = slot(2, 0, 0), slot(2, 0, 1)
    p_a, p_b = slot(0, 1, 0), slot(0, 1, 1)
    pl_a, pl_b, pr_a, pr_b = slot(3, 1, 0), slot(3, 1, 1), slot(1, 1, 0), slot(1, 1, 1)
    pll_a, pll_b = slot(2, 1, 0), slot(2, 1, 1)

    loads = [
        pltpu.make_async_copy(
            tokens.at[:, pl.ds(BLOCK * k, BLOCK)], tok.at[2 * own_a + k], load_sem.at[k]
        )
        for k in range(4)
    ]
    load_cot = pltpu.make_async_copy(cotangent, cot, load_sem.at[4])
    load_delta = pltpu.make_async_copy(delta, dbuf.at[z, c, yl], load_sem.at[5])
    load_cache = pltpu.make_async_copy(cache, weight, load_sem.at[6])
    for copy in (load_delta, *loads, load_cot, load_cache):
        copy.start()

    barrier = pltpu.get_barrier_semaphore()
    peers = [right, left, across, beside, sibling]
    peers += [{"z": (z + step) % NZ} for step in (1, 2, 6, 7)]
    for peer in peers:
        pl.semaphore_signal(barrier, inc=1, device_id=peer, device_id_type=MESH)
    pl.semaphore_wait(barrier, len(peers))

    way = {"right": (0, right), "left": (1, left), "across": (2, across)}

    def token_copy(place, direction, part=None):
        lane, peer = way[direction]
        first = 2 * place if part is None else 2 * place + part
        piece = pl.ds(first, 2 if part is None else 1)
        return pltpu.make_async_remote_copy(
            src_ref=tok.at[piece], dst_ref=tok.at[piece],
            send_sem=tok_send.at[lane], recv_sem=tok_recv.at[first],
            device_id=peer, device_id_type=MESH,
        )

    def send(place, direction, part=None):
        token_copy(place, direction, part).start()

    def arrived(place, part=None):
        token_copy(place, "right", part).wait_recv()

    def d2d_copy(place):
        return pltpu.make_async_remote_copy(
            src_ref=gbuf.at[place, 1 - c], dst_ref=grcv.at[place],
            send_sem=d2d_send, recv_sem=d2d_recv.at[place],
            device_id=sibling, device_id_type=MESH,
        )

    def target(place):
        block = place // 2
        return block // 4, 2 * (block % 4) + place % 2

    def offset(place):
        return (z - target(place)[1] + NZ) % NZ

    def mid_copy(place):
        away = offset(place)
        rows, depth = target(place)
        far = jnp.where(away == 4, 1, 0)
        side = jnp.where(away == 3, 2, jnp.where(away == 5, 6, 2 + 4 * (place % 2)))
        return pltpu.make_async_remote_copy(
            src_ref=zsnd.at[place], dst_ref=zmid.at[rows, side // 4, far],
            send_sem=z_send.at[place], recv_sem=m_recv.at[rows, side // 4, far],
            device_id={"z": (depth + side) % NZ}, device_id_type=MESH,
        )

    def z_copy(place):
        rows, depth = target(place)
        away = offset(place)
        entry = jnp.where(away < 3, away - 1, away - 4)
        return pltpu.make_async_remote_copy(
            src_ref=zsnd.at[place], dst_ref=zrcv.at[rows, entry],
            send_sem=z_send.at[place], recv_sem=z_recv.at[rows, entry],
            device_id={"z": depth}, device_id_type=MESH,
        )

    def pick(places, i):
        value = places[0]
        for k in range(1, len(places)):
            value = jnp.where(i == k, places[k], value)
        return value

    late = (pr_a, pr_b, pll_a, pl_b, pll_b)

    def is_late(place):
        found = place == late[0]
        for other in late[1:]:
            found = found | (place == other)
        return found

    def late_index(place):
        index = 0
        for k in range(1, len(late)):
            index = jnp.where(place == late[k], k, index)
        return index

    def late_copy(place):
        k = late_index(place)
        return pltpu.make_async_remote_copy(
            src_ref=zsnd.at[place], dst_ref=yin.at[k],
            send_sem=late_send.at[k], recv_sem=late_recv.at[k],
            device_id=beside, device_id_type=MESH,
        )

    def dispatch(place, total):
        away = offset(place)
        zsnd[place] = total.astype(BF16)

        @pl.when((away == 1) | (away == 7))
        def _():
            z_copy(place).start()

        @pl.when((away >= 3) & (away <= 5))
        def _():
            mid_copy(place).start()

        @pl.when((away == 2) | (away == 6))
        def _():
            gbuf[place, c] = total

        @pl.when(away == 0)
        def _():
            zloc[target(place)[0]] = total

    def merge(place):
        d2d_copy(place).wait_recv()
        dispatch(place, gbuf[place, c] + grcv[place])

    def merge_late(place):
        d2d_copy(place).wait_recv()
        total = gbuf[place, c] + grcv[place]

        @pl.when(target(place)[0] != yl)
        def _():
            zsnd[place] = total.astype(BF16)
            late_copy(place).start()

        @pl.when(target(place)[0] == yl)
        def _():
            gbuf[place, c] = total

    def finish_late(*places):
        def finish(i, carry):
            place = pick(places, i)

            @pl.when(target(place)[0] == yl)
            def _():
                late_copy(place).wait_recv()
                dispatch(place, gbuf[place, c] + yin[late_index(place)].astype(F32))

            return carry

        lax.fori_loop(0, len(places), finish, 0)

    def gradients(*places, combine=merge):
        def product(i, carry):
            place = pick(places, i)
            both = jnp.concatenate([tok[2 * place], tok[2 * place + 1]], axis=1)
            terms = jnp.dot(cot_t[...], both, preferred_element_type=F32)
            gbuf[place, 0] = terms[:, :BLOCK]
            gbuf[place, 1] = terms[:, BLOCK:]
            d2d_copy(place).start()
            return carry

        def finish(i, carry):
            combine(pick(places, i))
            return carry

        lax.fori_loop(0, len(places), product, 0)
        lax.fori_loop(0, len(places), finish, 0)

    def quarters(part, *places):
        def product(i, carry):
            place = pick(places, i)
            arrived(place, part)
            terms = jnp.dot(cot_t[...], tok[2 * place + part], preferred_element_type=F32)
            gbuf[place, part] = terms

            @pl.when(c != part)
            def _():
                d2d_copy(place).start()

            return carry

        def finish(i, carry):
            @pl.when(c == part)
            def _():
                merge_late(pick(places, i))

            return carry

        lax.fori_loop(0, len(places), product, 0)
        lax.fori_loop(0, len(places), finish, 0)

    def relays(*places, everywhere=True):
        def relay(i, carry):
            place = pick(places, i)
            here = everywhere | (target(place)[0] == yl)
            away = jnp.where(here, offset(place), 0)

            rows, side = target(place)[0], away // 4

            def inflow(far):
                return pltpu.make_async_remote_copy(
                    src_ref=zmid.at[rows, side, far], dst_ref=zmid.at[rows, side, far],
                    send_sem=z_send.at[place], recv_sem=m_recv.at[rows, side, far],
                    device_id=up, device_id_type=MESH,
                )

            @pl.when(away == 2 + 4 * (place % 2))
            def _():
                inflow(1).wait_recv()
                gbuf[place, c] += zmid[rows, side, 1].astype(F32)

            @pl.when((away == 2) | (away == 6))
            def _():
                inflow(0).wait_recv()
                zsnd[place] = (gbuf[place, c] + zmid[rows, side, 0].astype(F32)).astype(BF16)
                z_copy(place).start()

            return carry

        lax.fori_loop(0, len(places), relay, 0)

    def dz_copy(origin, peer):
        return pltpu.make_async_remote_copy(
            src_ref=dbuf.at[origin, c], dst_ref=dbuf.at[origin, c],
            send_sem=dz_send, recv_sem=dz_recv.at[origin],
            device_id=peer, device_id_type=MESH,
        )

    def dc_copy(origin):
        return pltpu.make_async_remote_copy(
            src_ref=dbuf.at[origin, c], dst_ref=dbuf.at[origin, c],
            send_sem=dc_send, recv_sem=dc_recv,
            device_id=sibling, device_id_type=MESH,
        )

    dy_copy = pltpu.make_async_remote_copy(
        src_ref=dbuf.at[z, c, yl], dst_ref=dbuf.at[z, c, yl],
        send_sem=dy_sem.at[0], recv_sem=dy_sem.at[1],
        device_id=beside, device_id_type=MESH,
    )
    dy_in = pltpu.make_async_remote_copy(
        src_ref=dbuf.at[z, c, 1 - yl], dst_ref=dbuf.at[z, c, 1 - yl],
        send_sem=dy_sem.at[0], recv_sem=dy_sem.at[1],
        device_id=beside, device_id_type=MESH,
    )

    def delta_step(step):
        below, above = (z + NZ - step) % NZ, (z + step) % NZ
        if step == 0:
            dy_in.wait_recv()
        else:
            dz_copy(below, up).wait_recv()
        if step < 4:
            dz_copy(below, up).start()
        dc_copy(below).start()
        if 0 < step < 4:
            dz_copy(above, down).wait_recv()
        if step < 3:
            dz_copy(above, down).start()
        if 0 < step < 4:
            dc_copy(above).start()

    def rebuild(j, carry):
        rows = pl.ds(pl.multiple_of(j * BLOCK, BLOCK), BLOCK)
        change = dbuf[(j % 16) // 2, j % 2, j // 16]
        weight[rows, :] = (weight[rows, :].astype(F32) + change.astype(F32)).astype(BF16)
        return carry

    def project(*firsts):
        def add(i, carry):
            first = pick(firsts, i)
            rows = pl.ds(pl.multiple_of(first * HALF, HALF), 2 * HALF)
            block = jnp.concatenate([tok[2 * first + k] for k in range(4)], axis=1)
            act[...] += jnp.dot(block, weight[rows, :], preferred_element_type=F32)
            return carry

        lax.fori_loop(0, len(firsts), add, 0)

    load_delta.wait()
    dy_copy.start()
    loads[0].wait()
    loads[1].wait()
    send(own_a, "right")
    send(own_a, "across")
    loads[2].wait()
    loads[3].wait()
    send(own_b, "left")
    send(own_b, "right")
    send(own_a, "left")
    load_cot.wait()
    cot_t[...] = cot[...].T
    gradients(own_a, own_b)
    delta_step(0)
    act[...] = jnp.zeros_like(act)

    arrived(l_a)
    send(l_a, "right")
    send(l_a, "across")
    send(own_b, "across")
    arrived(r_b)
    send(r_b, "left")
    send(r_b, "across", 0)
    send(r_b, "across", 1)
    arrived(p_a)
    send(p_a, "left")
    delta_step(1)
    gradients(l_a, r_b, p_a)
    relays(own_a, own_b)

    arrived(l_b)
    arrived(r_a)
    arrived(pl_a)
    send(pl_a, "right")
    delta_step(2)
    gradients(l_b, r_a, pl_a)
    relays(l_a, r_b, p_a)

    arrived(ll_a)
    arrived(ll_b)
    arrived(p_b)
    send(p_b, "right", 0)
    send(p_b, "right", 1)
    delta_step(3)
    gradients(ll_a, ll_b, p_b)
    relays(l_b, r_a, pl_a)

    arrived(pr_b, 0)
    send(pr_b, "left", 0)
    arrived(pr_a)
    arrived(pll_a)
    gradients(pr_a, pll_a, combine=merge_late)
    arrived(pr_b, 1)
    send(pr_b, "left", 1)
    gradients(pr_b, combine=merge_late)
    relays(ll_a, ll_b, p_b)
    delta_step(4)

    quarters(0, pl_b, pll_b)
    load_cache.wait()
    pltpu.make_async_remote_copy(
        src_ref=dbuf.at[:, 1 - c], dst_ref=dbuf.at[:, 1 - c],
        send_sem=dc_send, recv_sem=dc_recv,
        device_id=sibling, device_id_type=MESH,
    ).wait_recv()
    finish_late(pr_a, pll_a)
    lax.fori_loop(0, 32, rebuild, 0)
    quarters(1, pl_b, pll_b)
    finish_late(pr_b)
    project(own_a, l_a)
    finish_late(pl_b, pll_b)

    def collected(rows):
        total = zloc[rows]
        for entry in range(4):
            pltpu.make_async_remote_copy(
                src_ref=zrcv.at[rows, entry], dst_ref=zrcv.at[rows, entry],
                send_sem=z_send.at[0], recv_sem=z_recv.at[rows, entry],
                device_id=up, device_id_type=MESH,
            ).wait_recv()
            total = total + zrcv[rows, entry].astype(F32)
        return total

    mine, other = [8 * row + z for row in (yl, 1 - yl)]
    y_copy = pltpu.make_async_remote_copy(
        src_ref=ysnd, dst_ref=yrcv, send_sem=y_send, recv_sem=y_recv,
        device_id=beside, device_id_type=MESH,
    )
    early_out, early_in = jnp.logical_not(is_late(other)), jnp.logical_not(is_late(mine))

    @pl.when(early_out)
    def _():
        ysnd[...] = collected(1 - yl).astype(BF16)
        y_copy.start()

    relays(pr_a, pr_b, pll_a, everywhere=False)
    project(r_a, p_a)
    relays(pl_b, pll_b, everywhere=False)
    project(ll_a, pr_a, pl_a, pll_a)

    grad[...] = collected(yl)

    @pl.when(early_in)
    def _():
        y_copy.wait_recv()
        grad[...] += yrcv[...].astype(F32)


    @pl.when(early_out)
    def _():
        y_copy.wait_send()

    dy_copy.wait_send()
    def sent(block, sem):
        pltpu.make_async_remote_copy(
            src_ref=block, dst_ref=block, send_sem=sem, recv_sem=y_recv,
            device_id=beside, device_id_type=MESH,
        ).wait_send()

    sent(tok.at[pl.ds(0, 10)], tok_send.at[0])
    sent(tok.at[pl.ds(0, 10)], tok_send.at[1])
    sent(tok.at[pl.ds(0, 8)], tok_send.at[2])
    sent(dbuf.at[pl.ds(0, 7), c], dz_send)
    sent(dbuf.at[:, c], dc_send)
    sent(grcv, d2d_send)

    def drain(place, carry):
        aside = is_late(place) & (target(place)[0] != yl)

        @pl.when(aside)
        def _():
            late_copy(place).wait_send()

        @pl.when(jnp.logical_not(aside) & (offset(place) != 0))
        def _():
            sent(zsnd.at[place], z_send.at[place])

        return carry

    lax.fori_loop(0, 16, drain, 0)


def hadamard(length):
    first = lax.broadcasted_iota(jnp.int32, (length, length), 0)
    second = lax.broadcasted_iota(jnp.int32, (length, length), 1)
    common = jnp.bitwise_and(first, second)
    parity = jnp.zeros((length, length), jnp.int32)
    for place in range(length.bit_length() - 1):
        parity = parity + jnp.bitwise_and(jnp.right_shift(common, place), 1)
    signs = (1 - 2 * jnp.bitwise_and(parity, 1)).astype(F32)
    return signs / np.sqrt(np.float32(length))


def update(
    act_in, grad, bits, master, moment, variance,
    act, new_master, new_moment, new_variance, scales,
    out, peaks, sem_act, sem_out,
):
    move = pltpu.make_async_copy(act_in, act, sem_act)
    move.start()
    table = hadamard(BLOCK)
    for k in range(master.shape[1] // BLOCK):
        span = pl.ds(k * BLOCK, BLOCK)
        signs = (1 - 2 * bits[:, span]).astype(F32)
        gradient = grad[span, :].T
        smoothed = jnp.dot(
            gradient * signs, table, precision=lax.Precision.HIGHEST, preferred_element_type=F32
        )
        peaks[pl.ds(k, 1), :] = jnp.max(jnp.abs(smoothed.T), axis=0, keepdims=True)
        restored = signs * jnp.dot(
            smoothed, table, precision=lax.Precision.HIGHEST, preferred_element_type=F32
        )
        first = 0.9 * moment[:, span] + 0.1 * restored
        second = 0.95 * variance[:, span] + 0.05 * restored * restored
        corrected = first / (1.0 - 0.9**10)
        spread = jnp.sqrt(second / (1.0 - 0.95**10)) + 1e-08
        weight = master[:, span]
        out[0, :, span] = weight - 0.01 * (corrected / spread + 0.1 * weight)
        out[1, :, span] = first
        out[2, :, span] = second
    stores = [
        pltpu.make_async_copy(out.at[k], target, sem_out.at[k])
        for k, target in enumerate((new_master, new_moment, new_variance))
    ]
    stores.append(pltpu.make_async_copy(peaks, scales, sem_out.at[3]))
    for copy in stores:
        copy.start()
    move.wait()
    for copy in stores:
        copy.wait()


def body(tokens, cotangent, weight_cache, weight_delta, sign_bits, master, moment, variance):
    count, width = tokens.shape
    columns = cotangent.shape[1]
    inside = pl.BlockSpec(memory_space=pltpu.VMEM)
    outside = pl.BlockSpec(memory_space=pltpu.HBM)
    dma = pltpu.SemaphoreType.DMA
    piece = (columns, BLOCK)
    act, grad_t = pl.pallas_call(
        transport,
        out_shape=(
            jax.ShapeDtypeStruct((count, columns), F32),
            jax.ShapeDtypeStruct(piece, F32),
        ),
        in_specs=[outside] * 4,
        out_specs=(inside, inside),
        scratch_shapes=[
            pltpu.VMEM((32, count, BLOCK), BF16),
            pltpu.VMEM((count, columns), BF16),
            pltpu.VMEM((columns, count), BF16),
            pltpu.VMEM(weight_cache.shape, BF16),
            pltpu.VMEM((NZ, 2, 2, BLOCK, columns), BF16),
            pltpu.VMEM((16, 2, *piece), F32),
            pltpu.VMEM((16, *piece), F32),
            pltpu.VMEM((16, *piece), BF16),
            pltpu.VMEM((2, 2, 2, *piece), BF16),
            pltpu.VMEM((2, 4, *piece), BF16),
            pltpu.VMEM((2, *piece), F32),
            pltpu.VMEM(piece, BF16),
            pltpu.VMEM(piece, BF16),
            pltpu.VMEM((5, *piece), BF16),
            dma((7,)), dma((3,)), dma((32,)), dma, dma((16,)), dma((16,)),
            dma((2, 2, 2)), dma((2, 4)), dma, dma, dma((5,)), dma((5,)), dma((2,)), dma, dma((NZ,)), dma, dma,
        ],
        compiler_params=pltpu.CompilerParams(
            collective_id=0, has_side_effects=True, vmem_limit_bytes=46 * 2**20
        ),
        name="transport",
    )(*[pltpu.with_memory_space_constraint(a, pltpu.HBM) for a in (tokens, cotangent, weight_cache, weight_delta)])
    small = jax.ShapeDtypeStruct(master.shape, F32)
    act, new_master, new_moment, new_variance, scales = pl.pallas_call(
        update,
        out_shape=(
            jax.ShapeDtypeStruct((count, columns), F32),
            small, small, small,
            jax.ShapeDtypeStruct((columns // BLOCK, master.shape[0]), F32),
        ),
        in_specs=[inside] * 6,
        out_specs=(outside,) * 5,
        scratch_shapes=[
            pltpu.VMEM((3, *master.shape), F32),
            pltpu.VMEM((columns // BLOCK, master.shape[0]), F32),
            dma, dma((4,)),
        ],
        compiler_params=pltpu.CompilerParams(vmem_limit_bytes=10 * 2**20),
        name="update",
    )(act, grad_t, sign_bits.reshape(1, columns), master, moment, variance)
    return act, new_master, new_moment, new_variance, scales.T


def solution(mesh):
    torus = Mesh(mesh.devices.reshape(NX, 2, 2, NZ, 2), OUTER + INNER)
    split = P(INNER, OUTER)
    return jax.shard_map(
        body, mesh=torus,
        in_specs=(split, split, P(None, OUTER), split, P(OUTER), split, split, split),
        out_specs=(split,) * 5,
        check_vma=False,
    )
```

```python
import functools

import jax
import jax.numpy as jnp
import numpy as np
from jax import lax
from jax.experimental import pallas as pl
from jax.experimental.pallas import tpu as pltpu
from jax.sharding import Mesh
from jax.sharding import PartitionSpec as P

BLOCK = 128
OUTER = ("x", "yh")
INNER = ("yl", "z", "c")
NX, NZ = 4, 8
HALF = 256
MESH = pl.DeviceIdType.MESH
F32, BF16 = jnp.float32, jnp.bfloat16


def transport(
    tokens, cotangent, cache, delta,
    act, grad,
    tok, cot, cot_t, weight, dbuf, gbuf, grcv, zsnd, zmid, zrcv, zloc, ysnd, yrcv, yin,
    load_sem, tok_send, tok_recv, d2d_send, d2d_recv, z_send, m_recv, z_recv, y_send, y_recv,
    late_send, late_recv, dy_sem, dz_send, dz_recv, dc_send, dc_recv,
):
    x, yh, yl = lax.axis_index("x"), lax.axis_index("yh"), lax.axis_index("yl")
    z, c = lax.axis_index("z"), lax.axis_index("c")
    right, left = {"x": (x + 1) % NX}, {"x": (x + 3) % NX}
    across, beside, sibling = {"yh": 1 - yh}, {"yl": 1 - yl}, {"c": 1 - c}
    up, down = {"z": (z + 1) % NZ}, {"z": (z + 7) % NZ}

    def slot(dx, dy, half):
        row = yh if dy == 0 else 1 - yh
        return 4 * ((x + dx) % NX) + 2 * row + half

    own_a, own_b = slot(0, 0, 0), slot(0, 0, 1)
    l_a, l_b, r_a, r_b = slot(3, 0, 0), slot(3, 0, 1), slot(1, 0, 0), slot(1, 0, 1)
    ll_a, ll_b = slot(2, 0, 0), slot(2, 0, 1)
    p_a, p_b = slot(0, 1, 0), slot(0, 1, 1)
    pl_a, pl_b, pr_a, pr_b = slot(3, 1, 0), slot(3, 1, 1), slot(1, 1, 0), slot(1, 1, 1)
    pll_a, pll_b = slot(2, 1, 0), slot(2, 1, 1)

    loads = [
        pltpu.make_async_copy(
            tokens.at[:, pl.ds(BLOCK * k, BLOCK)], tok.at[2 * own_a + k], load_sem.at[k]
        )
        for k in range(4)
    ]
    load_cot = pltpu.make_async_copy(cotangent, cot, load_sem.at[4])
    load_delta = pltpu.make_async_copy(delta, dbuf.at[z, c, yl], load_sem.at[5])
    load_cache = pltpu.make_async_copy(cache, weight, load_sem.at[6])
    for copy in (load_delta, *loads, load_cot, load_cache):
        copy.start()

    barrier = pltpu.get_barrier_semaphore()
    peers = [right, left, across, beside, sibling]
    peers += [{"z": (z + step) % NZ} for step in (1, 2, 6, 7)]
    for peer in peers:
        pl.semaphore_signal(barrier, inc=1, device_id=peer, device_id_type=MESH)
    pl.semaphore_wait(barrier, len(peers))

    way = {"right": (0, right), "left": (1, left), "across": (2, across)}

    def token_copy(place, direction, part=None):
        lane, peer = way[direction]
        first = 2 * place if part is None else 2 * place + part
        piece = pl.ds(first, 2 if part is None else 1)
        return pltpu.make_async_remote_copy(
            src_ref=tok.at[piece], dst_ref=tok.at[piece],
            send_sem=tok_send.at[lane], recv_sem=tok_recv.at[first],
            device_id=peer, device_id_type=MESH,
        )

    def send(place, direction, part=None):
        token_copy(place, direction, part).start()

    def arrived(place, part=None):
        token_copy(place, "right", part).wait_recv()

    def d2d_copy(place):
        return pltpu.make_async_remote_copy(
            src_ref=gbuf.at[place, 1 - c], dst_ref=grcv.at[place],
            send_sem=d2d_send, recv_sem=d2d_recv.at[place],
            device_id=sibling, device_id_type=MESH,
        )

    def target(place):
        block = place // 2
        return block // 4, 2 * (block % 4) + place % 2

    def offset(place):
        return (z - target(place)[1] + NZ) % NZ

    def mid_copy(place):
        away = offset(place)
        rows, depth = target(place)
        far = jnp.where(away == 4, 1, 0)
        side = jnp.where(away == 3, 2, jnp.where(away == 5, 6, 2 + 4 * (place % 2)))
        return pltpu.make_async_remote_copy(
            src_ref=zsnd.at[place], dst_ref=zmid.at[rows, side // 4, far],
            send_sem=z_send.at[place], recv_sem=m_recv.at[rows, side // 4, far],
            device_id={"z": (depth + side) % NZ}, device_id_type=MESH,
        )

    def z_copy(place):
        rows, depth = target(place)
        away = offset(place)
        entry = jnp.where(away < 3, away - 1, away - 4)
        return pltpu.make_async_remote_copy(
            src_ref=zsnd.at[place], dst_ref=zrcv.at[rows, entry],
            send_sem=z_send.at[place], recv_sem=z_recv.at[rows, entry],
            device_id={"z": depth}, device_id_type=MESH,
        )

    def pick(places, i):
        value = places[0]
        for k in range(1, len(places)):
            value = jnp.where(i == k, places[k], value)
        return value

    late = (pr_a, pr_b, pll_a, pl_b, pll_b)

    def is_late(place):
        found = place == late[0]
        for other in late[1:]:
            found = found | (place == other)
        return found

    def late_index(place):
        index = 0
        for k in range(1, len(late)):
            index = jnp.where(place == late[k], k, index)
        return index

    def late_copy(place):
        k = late_index(place)
        return pltpu.make_async_remote_copy(
            src_ref=zsnd.at[place], dst_ref=yin.at[k],
            send_sem=late_send.at[k], recv_sem=late_recv.at[k],
            device_id=beside, device_id_type=MESH,
        )

    def dispatch(place, total):
        away = offset(place)
        zsnd[place] = total.astype(BF16)

        @pl.when((away == 1) | (away == 7))
        def _():
            z_copy(place).start()

        @pl.when((away >= 3) & (away <= 5))
        def _():
            mid_copy(place).start()

        @pl.when((away == 2) | (away == 6))
        def _():
            gbuf[place, c] = total

        @pl.when(away == 0)
        def _():
            zloc[target(place)[0]] = total

    def merge(place):
        d2d_copy(place).wait_recv()
        dispatch(place, gbuf[place, c] + grcv[place])

    def merge_late(place):
        d2d_copy(place).wait_recv()
        total = gbuf[place, c] + grcv[place]

        @pl.when(target(place)[0] != yl)
        def _():
            zsnd[place] = total.astype(BF16)
            late_copy(place).start()

        @pl.when(target(place)[0] == yl)
        def _():
            gbuf[place, c] = total

    def finish_late(*places):
        def finish(i, carry):
            place = pick(places, i)

            @pl.when(target(place)[0] == yl)
            def _():
                late_copy(place).wait_recv()
                dispatch(place, gbuf[place, c] + yin[late_index(place)].astype(F32))

            return carry

        lax.fori_loop(0, len(places), finish, 0)

    def gradients(*places, combine=merge):
        def product(i, carry):
            place = pick(places, i)
            both = jnp.concatenate([tok[2 * place], tok[2 * place + 1]], axis=1)
            terms = jnp.dot(cot_t[...], both, preferred_element_type=F32)
            gbuf[place, 0] = terms[:, :BLOCK]
            gbuf[place, 1] = terms[:, BLOCK:]
            d2d_copy(place).start()
            return carry

        def finish(i, carry):
            combine(pick(places, i))
            return carry

        lax.fori_loop(0, len(places), product, 0)
        lax.fori_loop(0, len(places), finish, 0)

    def quarters(part, *places, between=()):
        def product(i, carry):
            place = pick(places, i)
            arrived(place, part)
            terms = jnp.dot(cot_t[...], tok[2 * place + part], preferred_element_type=F32)
            gbuf[place, part] = terms

            @pl.when(c != part)
            def _():
                d2d_copy(place).start()

            return carry

        def finish(i, carry):
            @pl.when(c == part)
            def _():
                merge_late(pick(places, i))

            return carry

        lax.fori_loop(0, len(places), product, 0)
        if between:
            finish_late(*between)
        lax.fori_loop(0, len(places), finish, 0)

    def relays(*places, everywhere=True):
        def relay(i, carry):
            place = pick(places, i)
            here = everywhere | (target(place)[0] == yl)
            away = jnp.where(here, offset(place), 0)

            rows, side = target(place)[0], away // 4

            def inflow(far):
                return pltpu.make_async_remote_copy(
                    src_ref=zmid.at[rows, side, far], dst_ref=zmid.at[rows, side, far],
                    send_sem=z_send.at[place], recv_sem=m_recv.at[rows, side, far],
                    device_id=up, device_id_type=MESH,
                )

            @pl.when(away == 2 + 4 * (place % 2))
            def _():
                inflow(1).wait_recv()
                gbuf[place, c] += zmid[rows, side, 1].astype(F32)

            @pl.when((away == 2) | (away == 6))
            def _():
                inflow(0).wait_recv()
                zsnd[place] = (gbuf[place, c] + zmid[rows, side, 0].astype(F32)).astype(BF16)
                z_copy(place).start()

            return carry

        lax.fori_loop(0, len(places), relay, 0)

    def dz_copy(origin, peer):
        return pltpu.make_async_remote_copy(
            src_ref=dbuf.at[origin, c], dst_ref=dbuf.at[origin, c],
            send_sem=dz_send, recv_sem=dz_recv.at[origin],
            device_id=peer, device_id_type=MESH,
        )

    def dc_copy(origin):
        return pltpu.make_async_remote_copy(
            src_ref=dbuf.at[origin, c], dst_ref=dbuf.at[origin, c],
            send_sem=dc_send, recv_sem=dc_recv,
            device_id=sibling, device_id_type=MESH,
        )

    dy_copy = pltpu.make_async_remote_copy(
        src_ref=dbuf.at[z, c, yl], dst_ref=dbuf.at[z, c, yl],
        send_sem=dy_sem.at[0], recv_sem=dy_sem.at[1],
        device_id=beside, device_id_type=MESH,
    )
    dy_in = pltpu.make_async_remote_copy(
        src_ref=dbuf.at[z, c, 1 - yl], dst_ref=dbuf.at[z, c, 1 - yl],
        send_sem=dy_sem.at[0], recv_sem=dy_sem.at[1],
        device_id=beside, device_id_type=MESH,
    )

    def delta_step(step):
        below, above = (z + NZ - step) % NZ, (z + step) % NZ
        if step == 0:
            dy_in.wait_recv()
        else:
            dz_copy(below, up).wait_recv()
        if step < 4:
            dz_copy(below, up).start()
        dc_copy(below).start()
        if 0 < step < 4:
            dz_copy(above, down).wait_recv()
        if step < 3:
            dz_copy(above, down).start()
        if 0 < step < 4:
            dc_copy(above).start()

    def rebuild(j, carry):
        rows = pl.ds(pl.multiple_of(j * BLOCK, BLOCK), BLOCK)
        change = dbuf[(j % 16) // 2, j % 2, j // 16]
        weight[rows, :] = (weight[rows, :].astype(F32) + change.astype(F32)).astype(BF16)
        return carry

    def project(*firsts):
        def add(i, carry):
            first = pick(firsts, i)
            rows = pl.ds(pl.multiple_of(first * HALF, HALF), 2 * HALF)
            block = jnp.concatenate([tok[2 * first + k] for k in range(4)], axis=1)
            act[...] += jnp.dot(block, weight[rows, :], preferred_element_type=F32)
            return carry

        lax.fori_loop(0, len(firsts), add, 0)

    load_delta.wait()
    dy_copy.start()
    loads[0].wait()
    loads[1].wait()
    send(own_a, "right")
    send(own_a, "across")
    loads[2].wait()
    loads[3].wait()
    send(own_b, "left")
    send(own_b, "right")
    send(own_a, "left")
    load_cot.wait()
    cot_t[...] = cot[...].T
    gradients(own_a, own_b)
    delta_step(0)
    act[...] = jnp.zeros_like(act)

    arrived(l_a)
    send(l_a, "right")
    send(l_a, "across")
    send(own_b, "across")
    arrived(r_b)
    send(r_b, "left")
    send(r_b, "across", 0)
    send(r_b, "across", 1)
    arrived(p_a)
    send(p_a, "left")
    delta_step(1)
    gradients(l_a, r_b, p_a)
    relays(own_a, own_b)

    arrived(l_b)
    arrived(r_a)
    arrived(pl_a)
    send(pl_a, "right")
    delta_step(2)
    gradients(l_b, r_a, pl_a)
    relays(l_a, r_b, p_a)

    arrived(ll_a)
    arrived(ll_b)
    arrived(p_b)
    send(p_b, "right", 0)
    send(p_b, "right", 1)
    delta_step(3)
    gradients(ll_a, ll_b, p_b)
    relays(l_b, r_a, pl_a)

    arrived(pr_b, 0)
    send(pr_b, "left", 0)
    arrived(pr_a)
    arrived(pll_a)
    gradients(pr_a, pll_a, combine=merge_late)
    arrived(pr_b, 1)
    send(pr_b, "left", 1)
    gradients(pr_b, combine=merge_late)
    relays(ll_a, ll_b, p_b)
    delta_step(4)

    quarters(0, pl_b, pll_b)
    load_cache.wait()
    pltpu.make_async_remote_copy(
        src_ref=dbuf.at[:, 1 - c], dst_ref=dbuf.at[:, 1 - c],
        send_sem=dc_send, recv_sem=dc_recv,
        device_id=sibling, device_id_type=MESH,
    ).wait_recv()
    finish_late(pr_a, pll_a)
    lax.fori_loop(0, 32, rebuild, 0)
    quarters(1, pl_b, pll_b, between=(pr_b,))
    project(own_a, l_a)
    finish_late(pl_b, pll_b)

    def collected(rows):
        total = zloc[rows]
        for entry in range(4):
            pltpu.make_async_remote_copy(
                src_ref=zrcv.at[rows, entry], dst_ref=zrcv.at[rows, entry],
                send_sem=z_send.at[0], recv_sem=z_recv.at[rows, entry],
                device_id=up, device_id_type=MESH,
            ).wait_recv()
            total = total + zrcv[rows, entry].astype(F32)
        return total

    mine, other = [8 * row + z for row in (yl, 1 - yl)]
    y_copy = pltpu.make_async_remote_copy(
        src_ref=ysnd, dst_ref=yrcv, send_sem=y_send, recv_sem=y_recv,
        device_id=beside, device_id_type=MESH,
    )
    early_out, early_in = jnp.logical_not(is_late(other)), jnp.logical_not(is_late(mine))

    @pl.when(early_out)
    def _():
        ysnd[...] = collected(1 - yl).astype(BF16)
        y_copy.start()

    relays(pr_a, pr_b, pll_a, everywhere=False)
    project(r_a, p_a)
    relays(pl_b, pll_b, everywhere=False)
    project(ll_a, pr_a, pl_a, pll_a)

    @pl.when(early_out)
    def _():
        y_copy.wait_send()

    dy_copy.wait_send()
    def sent(block, sem):
        pltpu.make_async_remote_copy(
            src_ref=block, dst_ref=block, send_sem=sem, recv_sem=y_recv,
            device_id=beside, device_id_type=MESH,
        ).wait_send()

    sent(tok.at[pl.ds(0, 10)], tok_send.at[0])
    sent(tok.at[pl.ds(0, 10)], tok_send.at[1])
    sent(tok.at[pl.ds(0, 8)], tok_send.at[2])
    sent(dbuf.at[pl.ds(0, 7), c], dz_send)
    sent(dbuf.at[:, c], dc_send)
    sent(grcv, d2d_send)

    def drain(place, carry):
        aside = is_late(place) & (target(place)[0] != yl)

        @pl.when(aside)
        def _():
            late_copy(place).wait_send()

        @pl.when(jnp.logical_not(aside) & (offset(place) != 0))
        def _():
            sent(zsnd.at[place], z_send.at[place])

        return carry

    lax.fori_loop(0, 16, drain, 0)

    grad[...] = collected(yl)

    @pl.when(early_in)
    def _():
        y_copy.wait_recv()
        grad[...] += yrcv[...].astype(F32)


def hadamard(length):
    first = lax.broadcasted_iota(jnp.int32, (length, length), 0)
    second = lax.broadcasted_iota(jnp.int32, (length, length), 1)
    common = jnp.bitwise_and(first, second)
    parity = jnp.zeros((length, length), jnp.int32)
    for place in range(length.bit_length() - 1):
        parity = parity + jnp.bitwise_and(jnp.right_shift(common, place), 1)
    signs = (1 - 2 * jnp.bitwise_and(parity, 1)).astype(F32)
    return signs / np.sqrt(np.float32(length))


def update(
    act_in, grad, bits, master, moment, variance,
    act, new_master, new_moment, new_variance, scales,
    out, peaks, sem_act, sem_out,
):
    move = pltpu.make_async_copy(act_in, act, sem_act)
    move.start()
    table = hadamard(BLOCK)
    for k in range(master.shape[1] // BLOCK):
        span = pl.ds(k * BLOCK, BLOCK)
        signs = (1 - 2 * bits[:, span]).astype(F32)
        gradient = grad[span, :].T
        smoothed = jnp.dot(
            gradient * signs, table, precision=lax.Precision.HIGHEST, preferred_element_type=F32
        )
        peaks[pl.ds(k, 1), :] = jnp.max(jnp.abs(smoothed.T), axis=0, keepdims=True)
        restored = signs * jnp.dot(
            smoothed, table, precision=lax.Precision.HIGHEST, preferred_element_type=F32
        )
        first = 0.9 * moment[:, span] + 0.1 * restored
        second = 0.95 * variance[:, span] + 0.05 * restored * restored
        corrected = first / (1.0 - 0.9**10)
        spread = jnp.sqrt(second / (1.0 - 0.95**10)) + 1e-08
        weight = master[:, span]
        out[0, :, span] = weight - 0.01 * (corrected / spread + 0.1 * weight)
        out[1, :, span] = first
        out[2, :, span] = second
    stores = [
        pltpu.make_async_copy(out.at[k], target, sem_out.at[k])
        for k, target in enumerate((new_master, new_moment, new_variance))
    ]
    stores.append(pltpu.make_async_copy(peaks, scales, sem_out.at[3]))
    for copy in stores:
        copy.start()
    move.wait()
    for copy in stores:
        copy.wait()


def body(tokens, cotangent, weight_cache, weight_delta, sign_bits, master, moment, variance):
    count, width = tokens.shape
    columns = cotangent.shape[1]
    inside = pl.BlockSpec(memory_space=pltpu.VMEM)
    outside = pl.BlockSpec(memory_space=pltpu.HBM)
    dma = pltpu.SemaphoreType.DMA
    piece = (columns, BLOCK)
    act, grad_t = pl.pallas_call(
        transport,
        out_shape=(
            jax.ShapeDtypeStruct((count, columns), F32),
            jax.ShapeDtypeStruct(piece, F32),
        ),
        in_specs=[outside] * 4,
        out_specs=(inside, inside),
        scratch_shapes=[
            pltpu.VMEM((32, count, BLOCK), BF16),
            pltpu.VMEM((count, columns), BF16),
            pltpu.VMEM((columns, count), BF16),
            pltpu.VMEM(weight_cache.shape, BF16),
            pltpu.VMEM((NZ, 2, 2, BLOCK, columns), BF16),
            pltpu.VMEM((16, 2, *piece), F32),
            pltpu.VMEM((16, *piece), F32),
            pltpu.VMEM((16, *piece), BF16),
            pltpu.VMEM((2, 2, 2, *piece), BF16),
            pltpu.VMEM((2, 4, *piece), BF16),
            pltpu.VMEM((2, *piece), F32),
            pltpu.VMEM(piece, BF16),
            pltpu.VMEM(piece, BF16),
            pltpu.VMEM((5, *piece), BF16),
            dma((7,)), dma((3,)), dma((32,)), dma, dma((16,)), dma((16,)),
            dma((2, 2, 2)), dma((2, 4)), dma, dma, dma((5,)), dma((5,)), dma((2,)), dma, dma((NZ,)), dma, dma,
        ],
        compiler_params=pltpu.CompilerParams(
            collective_id=0, has_side_effects=True, vmem_limit_bytes=46 * 2**20
        ),
        name="transport",
    )(*[pltpu.with_memory_space_constraint(a, pltpu.HBM) for a in (tokens, cotangent, weight_cache, weight_delta)])
    small = jax.ShapeDtypeStruct(master.shape, F32)
    act, new_master, new_moment, new_variance, scales = pl.pallas_call(
        update,
        out_shape=(
            jax.ShapeDtypeStruct((count, columns), F32),
            small, small, small,
            jax.ShapeDtypeStruct((columns // BLOCK, master.shape[0]), F32),
        ),
        in_specs=[inside] * 6,
        out_specs=(outside,) * 5,
        scratch_shapes=[
            pltpu.VMEM((3, *master.shape), F32),
            pltpu.VMEM((columns // BLOCK, master.shape[0]), F32),
            dma, dma((4,)),
        ],
        compiler_params=pltpu.CompilerParams(vmem_limit_bytes=10 * 2**20),
        name="update",
    )(act, grad_t, sign_bits.reshape(1, columns), master, moment, variance)
    return act, new_master, new_moment, new_variance, scales.T


def solution(mesh):
    torus = Mesh(mesh.devices.reshape(NX, 2, 2, NZ, 2), OUTER + INNER)
    split = P(INNER, OUTER)
    return jax.shard_map(
        body, mesh=torus,
        in_specs=(split, split, P(None, OUTER), split, P(OUTER), split, split, split),
        out_specs=(split,) * 5,
        check_vma=False,
    )
```

```python
import functools

import jax
import jax.numpy as jnp
import numpy as np
from jax import lax
from jax.experimental import pallas as pl
from jax.experimental.pallas import tpu as pltpu
from jax.sharding import Mesh
from jax.sharding import PartitionSpec as P

BLOCK = 128
OUTER = ("x", "yh")
INNER = ("yl", "z", "c")
NX, NZ = 4, 8
HALF = 256
MESH = pl.DeviceIdType.MESH
F32, BF16 = jnp.float32, jnp.bfloat16


def transport(
    tokens, cotangent, cache, delta,
    act, grad,
    tok, cot, cot_t, weight, dbuf, gbuf, grcv, zsnd, zmid, zrcv, zloc, ysnd, yrcv, yin,
    load_sem, tok_send, tok_recv, d2d_send, d2d_recv, z_send, m_recv, z_recv, y_send, y_recv,
    late_send, late_recv, dy_sem, dz_send, dz_recv, dc_send, dc_recv,
):
    x, yh, yl = lax.axis_index("x"), lax.axis_index("yh"), lax.axis_index("yl")
    z, c = lax.axis_index("z"), lax.axis_index("c")
    right, left = {"x": (x + 1) % NX}, {"x": (x + 3) % NX}
    across, beside, sibling = {"yh": 1 - yh}, {"yl": 1 - yl}, {"c": 1 - c}
    up, down = {"z": (z + 1) % NZ}, {"z": (z + 7) % NZ}

    def slot(dx, dy, half):
        row = yh if dy == 0 else 1 - yh
        return 4 * ((x + dx) % NX) + 2 * row + half

    own_a, own_b = slot(0, 0, 0), slot(0, 0, 1)
    l_a, l_b, r_a, r_b = slot(3, 0, 0), slot(3, 0, 1), slot(1, 0, 0), slot(1, 0, 1)
    ll_a, ll_b = slot(2, 0, 0), slot(2, 0, 1)
    p_a, p_b = slot(0, 1, 0), slot(0, 1, 1)
    pl_a, pl_b, pr_a, pr_b = slot(3, 1, 0), slot(3, 1, 1), slot(1, 1, 0), slot(1, 1, 1)
    pll_a, pll_b = slot(2, 1, 0), slot(2, 1, 1)

    loads = [
        pltpu.make_async_copy(
            tokens.at[:, pl.ds(BLOCK * k, BLOCK)], tok.at[2 * own_a + k], load_sem.at[k]
        )
        for k in range(4)
    ]
    load_cot = pltpu.make_async_copy(cotangent, cot, load_sem.at[4])
    load_delta = pltpu.make_async_copy(delta, dbuf.at[z, c, yl], load_sem.at[5])
    load_cache = pltpu.make_async_copy(cache, weight, load_sem.at[6])
    for copy in (load_delta, *loads, load_cot, load_cache):
        copy.start()

    barrier = pltpu.get_barrier_semaphore()
    peers = [right, left, across, beside, sibling]
    peers += [{"z": (z + step) % NZ} for step in (1, 2, 6, 7)]
    for peer in peers:
        pl.semaphore_signal(barrier, inc=1, device_id=peer, device_id_type=MESH)
    pl.semaphore_wait(barrier, len(peers))

    way = {"right": (0, right), "left": (1, left), "across": (2, across)}

    def token_copy(place, direction, part=None):
        lane, peer = way[direction]
        first = 2 * place if part is None else 2 * place + part
        piece = pl.ds(first, 2 if part is None else 1)
        return pltpu.make_async_remote_copy(
            src_ref=tok.at[piece], dst_ref=tok.at[piece],
            send_sem=tok_send.at[lane], recv_sem=tok_recv.at[first],
            device_id=peer, device_id_type=MESH,
        )

    def send(place, direction, part=None):
        token_copy(place, direction, part).start()

    def arrived(place, part=None):
        token_copy(place, "right", part).wait_recv()

    def d2d_copy(place):
        return pltpu.make_async_remote_copy(
            src_ref=gbuf.at[place, 1 - c], dst_ref=grcv.at[place],
            send_sem=d2d_send, recv_sem=d2d_recv.at[place],
            device_id=sibling, device_id_type=MESH,
        )

    def target(place):
        block = place // 2
        return block // 4, 2 * (block % 4) + place % 2

    def offset(place):
        return (z - target(place)[1] + NZ) % NZ

    def mid_copy(place):
        away = offset(place)
        rows, depth = target(place)
        far = jnp.where(away == 4, 1, 0)
        side = jnp.where(away == 3, 2, jnp.where(away == 5, 6, 2 + 4 * (place % 2)))
        return pltpu.make_async_remote_copy(
            src_ref=zsnd.at[place], dst_ref=zmid.at[rows, side // 4, far],
            send_sem=z_send.at[place], recv_sem=m_recv.at[rows, side // 4, far],
            device_id={"z": (depth + side) % NZ}, device_id_type=MESH,
        )

    def z_copy(place):
        rows, depth = target(place)
        away = offset(place)
        entry = jnp.where(away < 3, away - 1, away - 4)
        return pltpu.make_async_remote_copy(
            src_ref=zsnd.at[place], dst_ref=zrcv.at[rows, entry],
            send_sem=z_send.at[place], recv_sem=z_recv.at[rows, entry],
            device_id={"z": depth}, device_id_type=MESH,
        )

    def pick(places, i):
        value = places[0]
        for k in range(1, len(places)):
            value = jnp.where(i == k, places[k], value)
        return value

    late = (pr_a, pr_b, pll_a, pl_b, pll_b)

    def is_late(place):
        found = place == late[0]
        for other in late[1:]:
            found = found | (place == other)
        return found

    def late_index(place):
        index = 0
        for k in range(1, len(late)):
            index = jnp.where(place == late[k], k, index)
        return index

    def late_copy(place):
        k = late_index(place)
        return pltpu.make_async_remote_copy(
            src_ref=zsnd.at[place], dst_ref=yin.at[k],
            send_sem=late_send.at[k], recv_sem=late_recv.at[k],
            device_id=beside, device_id_type=MESH,
        )

    def dispatch(place, total):
        away = offset(place)
        zsnd[place] = total.astype(BF16)

        @pl.when((away == 1) | (away == 7))
        def _():
            z_copy(place).start()

        @pl.when((away >= 3) & (away <= 5))
        def _():
            mid_copy(place).start()

        @pl.when((away == 2) | (away == 6))
        def _():
            gbuf[place, c] = total

        @pl.when(away == 0)
        def _():
            zloc[target(place)[0]] = total

    def merge(place):
        d2d_copy(place).wait_recv()
        dispatch(place, gbuf[place, c] + grcv[place])

    def merge_late(place):
        d2d_copy(place).wait_recv()
        total = gbuf[place, c] + grcv[place]

        @pl.when(target(place)[0] != yl)
        def _():
            zsnd[place] = total.astype(BF16)
            late_copy(place).start()

        @pl.when(target(place)[0] == yl)
        def _():
            gbuf[place, c] = total

    def finish_late(*places):
        def finish(i, carry):
            place = pick(places, i)

            @pl.when(target(place)[0] == yl)
            def _():
                late_copy(place).wait_recv()
                dispatch(place, gbuf[place, c] + yin[late_index(place)].astype(F32))

            return carry

        lax.fori_loop(0, len(places), finish, 0)

    def gradients(*places, combine=merge):
        def product(i, carry):
            place = pick(places, i)
            both = jnp.concatenate([tok[2 * place], tok[2 * place + 1]], axis=1)
            terms = jnp.dot(cot_t[...], both, preferred_element_type=F32)
            gbuf[place, 0] = terms[:, :BLOCK]
            gbuf[place, 1] = terms[:, BLOCK:]
            d2d_copy(place).start()
            return carry

        def finish(i, carry):
            combine(pick(places, i))
            return carry

        lax.fori_loop(0, len(places), product, 0)
        lax.fori_loop(0, len(places), finish, 0)

    def quarters(part, *places, between=()):
        def product(i, carry):
            place = pick(places, i)
            arrived(place, part)
            terms = jnp.dot(cot_t[...], tok[2 * place + part], preferred_element_type=F32)
            gbuf[place, part] = terms

            @pl.when(c != part)
            def _():
                d2d_copy(place).start()

            return carry

        def finish(i, carry):
            @pl.when(c == part)
            def _():
                merge_late(pick(places, i))

            return carry

        lax.fori_loop(0, len(places), product, 0)
        if between:
            finish_late(*between)
        lax.fori_loop(0, len(places), finish, 0)

    def relays(*places, everywhere=True):
        def relay(i, carry):
            place = pick(places, i)
            here = everywhere | (target(place)[0] == yl)
            away = jnp.where(here, offset(place), 0)

            rows, side = target(place)[0], away // 4

            def inflow(far):
                return pltpu.make_async_remote_copy(
                    src_ref=zmid.at[rows, side, far], dst_ref=zmid.at[rows, side, far],
                    send_sem=z_send.at[place], recv_sem=m_recv.at[rows, side, far],
                    device_id=up, device_id_type=MESH,
                )

            @pl.when(away == 2 + 4 * (place % 2))
            def _():
                inflow(1).wait_recv()
                gbuf[place, c] += zmid[rows, side, 1].astype(F32)

            @pl.when((away == 2) | (away == 6))
            def _():
                inflow(0).wait_recv()
                zsnd[place] = (gbuf[place, c] + zmid[rows, side, 0].astype(F32)).astype(BF16)
                z_copy(place).start()

            return carry

        lax.fori_loop(0, len(places), relay, 0)

    def dz_copy(origin, peer):
        return pltpu.make_async_remote_copy(
            src_ref=dbuf.at[origin, c], dst_ref=dbuf.at[origin, c],
            send_sem=dz_send, recv_sem=dz_recv.at[origin],
            device_id=peer, device_id_type=MESH,
        )

    def dc_copy(origin):
        return pltpu.make_async_remote_copy(
            src_ref=dbuf.at[origin, c], dst_ref=dbuf.at[origin, c],
            send_sem=dc_send, recv_sem=dc_recv,
            device_id=sibling, device_id_type=MESH,
        )

    dy_copy = pltpu.make_async_remote_copy(
        src_ref=dbuf.at[z, c, yl], dst_ref=dbuf.at[z, c, yl],
        send_sem=dy_sem.at[0], recv_sem=dy_sem.at[1],
        device_id=beside, device_id_type=MESH,
    )
    dy_in = pltpu.make_async_remote_copy(
        src_ref=dbuf.at[z, c, 1 - yl], dst_ref=dbuf.at[z, c, 1 - yl],
        send_sem=dy_sem.at[0], recv_sem=dy_sem.at[1],
        device_id=beside, device_id_type=MESH,
    )

    def delta_step(step):
        below, above = (z + NZ - step) % NZ, (z + step) % NZ
        if step == 0:
            dy_in.wait_recv()
        else:
            dz_copy(below, up).wait_recv()
        if step < 4:
            dz_copy(below, up).start()
        dc_copy(below).start()
        if 0 < step < 4:
            dz_copy(above, down).wait_recv()
        if step < 3:
            dz_copy(above, down).start()
        if 0 < step < 4:
            dc_copy(above).start()

    def rebuild(j, carry):
        rows = pl.ds(pl.multiple_of(j * BLOCK, BLOCK), BLOCK)
        change = dbuf[(j % 16) // 2, j % 2, j // 16]
        weight[rows, :] = (weight[rows, :].astype(F32) + change.astype(F32)).astype(BF16)
        return carry

    def project(*firsts):
        def add(i, carry):
            first = pick(firsts, i)
            rows = pl.ds(pl.multiple_of(first * HALF, HALF), 2 * HALF)
            block = jnp.concatenate([tok[2 * first + k] for k in range(4)], axis=1)
            act[...] += jnp.dot(block, weight[rows, :], preferred_element_type=F32)
            return carry

        lax.fori_loop(0, len(firsts), add, 0)

    load_delta.wait()
    dy_copy.start()
    loads[0].wait()
    loads[1].wait()
    send(own_a, "right")
    send(own_a, "across")
    loads[2].wait()
    loads[3].wait()
    send(own_b, "left")
    send(own_b, "right")
    send(own_a, "left")
    load_cot.wait()
    cot_t[...] = cot[...].T
    gradients(own_a, own_b)
    delta_step(0)
    act[...] = jnp.zeros_like(act)

    arrived(l_a)
    send(l_a, "right")
    send(l_a, "across")
    send(own_b, "across")
    arrived(r_b)
    send(r_b, "left")
    send(r_b, "across", 0)
    send(r_b, "across", 1)
    arrived(p_a)
    send(p_a, "left")
    delta_step(1)
    gradients(l_a, r_b, p_a)
    relays(own_a, own_b)

    arrived(l_b)
    arrived(r_a)
    arrived(pl_a)
    send(pl_a, "right")
    delta_step(2)
    gradients(l_b, r_a, pl_a)
    relays(l_a, r_b, p_a)

    arrived(ll_a)
    arrived(ll_b)
    arrived(p_b)
    send(p_b, "right", 0)
    send(p_b, "right", 1)
    delta_step(3)
    gradients(ll_a, ll_b, p_b)
    relays(l_b, r_a, pl_a)

    arrived(pr_b, 0)
    send(pr_b, "left", 0)
    arrived(pr_a)
    arrived(pll_a)
    gradients(pr_a, pll_a, combine=merge_late)
    arrived(pr_b, 1)
    send(pr_b, "left", 1)
    gradients(pr_b, combine=merge_late)
    relays(ll_a, ll_b, p_b)
    delta_step(4)

    quarters(0, pl_b, pll_b)
    load_cache.wait()
    pltpu.make_async_remote_copy(
        src_ref=dbuf.at[:, 1 - c], dst_ref=dbuf.at[:, 1 - c],
        send_sem=dc_send, recv_sem=dc_recv,
        device_id=sibling, device_id_type=MESH,
    ).wait_recv()
    finish_late(pr_a, pll_a)
    lax.fori_loop(0, 32, rebuild, 0)
    quarters(1, pl_b, pll_b, between=(pr_b,))
    project(own_a, l_a)
    finish_late(pl_b, pll_b)

    def collected(rows):
        total = zloc[rows]
        for entry in range(4):
            pltpu.make_async_remote_copy(
                src_ref=zrcv.at[rows, entry], dst_ref=zrcv.at[rows, entry],
                send_sem=z_send.at[0], recv_sem=z_recv.at[rows, entry],
                device_id=up, device_id_type=MESH,
            ).wait_recv()
            total = total + zrcv[rows, entry].astype(F32)
        return total

    mine, other = [8 * row + z for row in (yl, 1 - yl)]
    y_copy = pltpu.make_async_remote_copy(
        src_ref=ysnd, dst_ref=yrcv, send_sem=y_send, recv_sem=y_recv,
        device_id=beside, device_id_type=MESH,
    )
    early_out, early_in = jnp.logical_not(is_late(other)), jnp.logical_not(is_late(mine))

    @pl.when(early_out)
    def _():
        ysnd[...] = collected(1 - yl).astype(BF16)
        y_copy.start()

    relays(pr_a, pr_b, pll_a, everywhere=False)
    project(r_a)
    relays(pl_b, pll_b, everywhere=False)
    project(p_a, ll_a, pr_a, pl_a, pll_a)

    @pl.when(early_out)
    def _():
        y_copy.wait_send()

    dy_copy.wait_send()
    def sent(block, sem):
        pltpu.make_async_remote_copy(
            src_ref=block, dst_ref=block, send_sem=sem, recv_sem=y_recv,
            device_id=beside, device_id_type=MESH,
        ).wait_send()

    sent(tok.at[pl.ds(0, 10)], tok_send.at[0])
    sent(tok.at[pl.ds(0, 10)], tok_send.at[1])
    sent(tok.at[pl.ds(0, 8)], tok_send.at[2])
    sent(dbuf.at[pl.ds(0, 7), c], dz_send)
    sent(dbuf.at[:, c], dc_send)
    sent(grcv, d2d_send)

    def drain(place, carry):
        aside = is_late(place) & (target(place)[0] != yl)

        @pl.when(aside)
        def _():
            late_copy(place).wait_send()

        @pl.when(jnp.logical_not(aside) & (offset(place) != 0))
        def _():
            sent(zsnd.at[place], z_send.at[place])

        return carry

    lax.fori_loop(0, 16, drain, 0)

    grad[...] = collected(yl)

    @pl.when(early_in)
    def _():
        y_copy.wait_recv()
        grad[...] += yrcv[...].astype(F32)


def hadamard(length):
    first = lax.broadcasted_iota(jnp.int32, (length, length), 0)
    second = lax.broadcasted_iota(jnp.int32, (length, length), 1)
    common = jnp.bitwise_and(first, second)
    parity = jnp.zeros((length, length), jnp.int32)
    for place in range(length.bit_length() - 1):
        parity = parity + jnp.bitwise_and(jnp.right_shift(common, place), 1)
    signs = (1 - 2 * jnp.bitwise_and(parity, 1)).astype(F32)
    return signs / np.sqrt(np.float32(length))


def update(
    act_in, grad, bits, master, moment, variance,
    act, new_master, new_moment, new_variance, scales,
    out, peaks, sem_act, sem_out,
):
    move = pltpu.make_async_copy(act_in, act, sem_act)
    move.start()
    table = hadamard(BLOCK)
    for k in range(master.shape[1] // BLOCK):
        span = pl.ds(k * BLOCK, BLOCK)
        signs = (1 - 2 * bits[:, span]).astype(F32)
        gradient = grad[span, :].T
        smoothed = jnp.dot(
            gradient * signs, table, precision=lax.Precision.HIGHEST, preferred_element_type=F32
        )
        peaks[pl.ds(k, 1), :] = jnp.max(jnp.abs(smoothed.T), axis=0, keepdims=True)
        restored = signs * jnp.dot(
            smoothed, table, precision=lax.Precision.HIGHEST, preferred_element_type=F32
        )
        first = 0.9 * moment[:, span] + 0.1 * restored
        second = 0.95 * variance[:, span] + 0.05 * restored * restored
        corrected = first / (1.0 - 0.9**10)
        spread = jnp.sqrt(second / (1.0 - 0.95**10)) + 1e-08
        weight = master[:, span]
        out[0, :, span] = weight - 0.01 * (corrected / spread + 0.1 * weight)
        out[1, :, span] = first
        out[2, :, span] = second
    stores = [
        pltpu.make_async_copy(out.at[k], target, sem_out.at[k])
        for k, target in enumerate((new_master, new_moment, new_variance))
    ]
    stores.append(pltpu.make_async_copy(peaks, scales, sem_out.at[3]))
    for copy in stores:
        copy.start()
    move.wait()
    for copy in stores:
        copy.wait()


def body(tokens, cotangent, weight_cache, weight_delta, sign_bits, master, moment, variance):
    count, width = tokens.shape
    columns = cotangent.shape[1]
    inside = pl.BlockSpec(memory_space=pltpu.VMEM)
    outside = pl.BlockSpec(memory_space=pltpu.HBM)
    dma = pltpu.SemaphoreType.DMA
    piece = (columns, BLOCK)
    act, grad_t = pl.pallas_call(
        transport,
        out_shape=(
            jax.ShapeDtypeStruct((count, columns), F32),
            jax.ShapeDtypeStruct(piece, F32),
        ),
        in_specs=[outside] * 4,
        out_specs=(inside, inside),
        scratch_shapes=[
            pltpu.VMEM((32, count, BLOCK), BF16),
            pltpu.VMEM((count, columns), BF16),
            pltpu.VMEM((columns, count), BF16),
            pltpu.VMEM(weight_cache.shape, BF16),
            pltpu.VMEM((NZ, 2, 2, BLOCK, columns), BF16),
            pltpu.VMEM((16, 2, *piece), F32),
            pltpu.VMEM((16, *piece), F32),
            pltpu.VMEM((16, *piece), BF16),
            pltpu.VMEM((2, 2, 2, *piece), BF16),
            pltpu.VMEM((2, 4, *piece), BF16),
            pltpu.VMEM((2, *piece), F32),
            pltpu.VMEM(piece, BF16),
            pltpu.VMEM(piece, BF16),
            pltpu.VMEM((5, *piece), BF16),
            dma((7,)), dma((3,)), dma((32,)), dma, dma((16,)), dma((16,)),
            dma((2, 2, 2)), dma((2, 4)), dma, dma, dma((5,)), dma((5,)), dma((2,)), dma, dma((NZ,)), dma, dma,
        ],
        compiler_params=pltpu.CompilerParams(
            collective_id=0, has_side_effects=True, vmem_limit_bytes=46 * 2**20
        ),
        name="transport",
    )(*[pltpu.with_memory_space_constraint(a, pltpu.HBM) for a in (tokens, cotangent, weight_cache, weight_delta)])
    small = jax.ShapeDtypeStruct(master.shape, F32)
    act, new_master, new_moment, new_variance, scales = pl.pallas_call(
        update,
        out_shape=(
            jax.ShapeDtypeStruct((count, columns), F32),
            small, small, small,
            jax.ShapeDtypeStruct((columns // BLOCK, master.shape[0]), F32),
        ),
        in_specs=[inside] * 6,
        out_specs=(outside,) * 5,
        scratch_shapes=[
            pltpu.VMEM((3, *master.shape), F32),
            pltpu.VMEM((columns // BLOCK, master.shape[0]), F32),
            dma, dma((4,)),
        ],
        compiler_params=pltpu.CompilerParams(vmem_limit_bytes=10 * 2**20),
        name="update",
    )(act, grad_t, sign_bits.reshape(1, columns), master, moment, variance)
    return act, new_master, new_moment, new_variance, scales.T


def solution(mesh):
    torus = Mesh(mesh.devices.reshape(NX, 2, 2, NZ, 2), OUTER + INNER)
    split = P(INNER, OUTER)
    return jax.shard_map(
        body, mesh=torus,
        in_specs=(split, split, P(None, OUTER), split, P(OUTER), split, split, split),
        out_specs=(split,) * 5,
        check_vma=False,
    )
```
